256 devices in a mesh: seq: 64 (over z, x, core), dp: 4 (over y).
Axes of the slice: x: 4, y: 4, z: 8, core: 2. Of those that a mesh axis runs over, the one named last changes fastest.
Arguments:
- conv_input: bfloat16 [4, 16384, 256], P('dp', 'seq'), may hold values from -6 to 6
- in_state_map: bfloat16 [4, 16384, 128], P('dp', 'seq'), may hold values from -6 to 6
- out_state_map: bfloat16 [4, 16384, 128], P('dp', 'seq'), may hold values from -1.25 to 1.25
- step_size: float32 [4, 16384, 4], P('dp', 'seq'), may hold values from 0.01 to 0.1
- decay_rate: float32 [4], replicated, may hold values from 0.00030517578 to 1.3
- skip_gain: float32 [4], replicated, may hold values from 0.5 to 1.5
- conv_weight: float32 [4, 256], replicated, may hold values from -3 to 3
- grad_mixer: bfloat16 [4, 16384, 256], P('dp', 'seq'), may hold values from -6 to 6
- grad_output: bfloat16 [4, 16384, 8192], P('dp', 'seq'), may hold values from -0.15625 to 0.15625
Outputs:
- grad_conv_input: bfloat16 [4, 16384, 256], P('dp', 'seq')
- grad_in_map: bfloat16 [4, 16384, 128], P('dp', 'seq')
- grad_out_map: bfloat16 [4, 16384, 128], P('dp', 'seq')
- grad_conv_weight: float32 [4, 256], replicated
- grad_out_proj: float32 [8192, 256], P(('seq', 'dp'))
The draws below stay inside these ranges and needn't reach their ends.
All inputs are finite; a program needn't handle non-finite values.
Results may differ from the reference program's by a relative error of at most 0.009.
Values may be sent and summed in bfloat16 or wider, within the bound.
A program may use at most 64 MiB of HBM per device.

```python
import math
import jax
import jax.numpy as jnp
from jax import lax

TOK_DEV = 256
HEADS = 4
HEAD_DIM = 64
STATE = 128
CONV = 4
OUT_FEATS = 8192
INNER = 256
SEQ = 16384
BATCH = 4
TOKENS = 65536


def draw_decay_rate(key, part):
    key_order = jax.random.fold_in(key, 11)
    key_slow = jax.random.fold_in(key, 12)
    key_fast = jax.random.fold_in(key, 13)
    ranking = jax.random.permutation(key_order, HEADS)
    mean_step = 0.039
    slow_rates = jnp.exp(jax.random.uniform(key_slow, (HEADS,), jnp.float32, jnp.log(0.2), jnp.log(1.5))) / (mean_step * SEQ)
    fast_rates = jnp.exp(jax.random.uniform(key_fast, (HEADS,), jnp.float32, jnp.log(0.025), jnp.log(0.05))) / mean_step
    slow_count = HEADS // 2
    return jnp.where(ranking < slow_count, slow_rates, fast_rates).astype(jnp.float32)


def with_spikes(entries, own_key, source, target, shards_of, factor):
    owner, partner = [(jnp.arange(entries.shape[dim]) // (entries.shape[dim] // shards_of)).reshape([-1 if axis == dim else 1 for axis in range(entries.ndim)]) for dim in (source, target)]
    chosen = jax.random.permutation(own_key, shards_of)[partner]
    strong = (owner == chosen) | (owner == (partner + shards_of // 2) % shards_of)
    return jnp.where(strong, factor * entries, entries)


def levels(key, dims, shards, least, top_value):
    level = 1.0
    for axis_at, shards_of in shards:
        steps = jax.random.uniform(jax.random.fold_in(jax.random.fold_in(key, 6), axis_at), (shards_of,), jnp.float32, least / len(shards), top_value / len(shards))
        level = level * jnp.repeat(jnp.exp(steps), dims[axis_at] // shards_of).reshape((-1,) + (1,) * (len(dims) - 1 - axis_at))
    return level


def centred(rng, shape, scale, most, cuts=(), kind=jnp.bfloat16):
    array = jax.random.normal(rng, shape, jnp.float32) * scale
    if len(cuts) > 0:
        array = levels(rng, shape, cuts, -0.22, 0.18) * array
    return jnp.clip(array, min=-most, max=most).astype(kind)


def bell_draw_with(own_key, shape, width, limit, shards, heavy, dtype=jnp.bfloat16):
    array = width * jax.random.normal(own_key, shape, jnp.float32)
    if shards:
        array = array * levels(own_key, shape, shards, -0.22, 0.18)
    return jnp.clip(with_spikes(array, jax.random.fold_in(own_key, 3), *heavy), -limit, limit).astype(dtype)


def setup_inputs(seed: int = 0) -> dict:
    arg_keys = jax.random.split(jax.random.key(seed), 10)
    conv_input = centred(arg_keys[0], (BATCH, SEQ, INNER), 1.0, 6.0, ((0, 4), (1, 64)))
    in_state_map = centred(arg_keys[1], (BATCH, SEQ, STATE), 1.0, 6.0, ((0, 4), (1, 64)))
    out_state_map = centred(arg_keys[2], (BATCH, SEQ, STATE), (STATE ** -0.5), 1.25, ((0, 4), (1, 64)))
    step_size = jnp.clip(jnp.exp(math.log(0.1) - 2.3025851 * jax.random.uniform(arg_keys[3], (BATCH, SEQ, HEADS), jnp.float32) ** levels(arg_keys[3], (BATCH, SEQ, HEADS), ((0, 4), (1, 64)), -0.2, 0.2)), 0.01, 0.1)
    decay_rate = draw_decay_rate(jax.random.fold_in(arg_keys[9], 71), 0)
    skip_gain = jnp.clip(jax.random.uniform(arg_keys[5], (HEADS,), jnp.float32, 0.5, 1.5), 0.5, 1.5)
    conv_weight = centred(arg_keys[6], (CONV, INNER), CONV ** -0.5, 3.0, (), jnp.float32)
    grad_mixer = centred(arg_keys[7], (BATCH, SEQ, INNER), 1.0, 6.0, ((0, 4), (1, 64)))
    grad_output = bell_draw_with(arg_keys[8], (BATCH, SEQ, OUT_FEATS), (TOKENS ** -0.5), 0.15625, ((0, 4), (1, 64)), (1, 2, 64, 4.0))
    return {"conv_input": conv_input, "in_state_map": in_state_map, "out_state_map": out_state_map, "step_size": step_size, "decay_rate": decay_rate, "skip_gain": skip_gain, "conv_weight": conv_weight, "grad_mixer": grad_mixer, "grad_output": grad_output}


highest = lax.Precision.HIGHEST


def product(left_side, right_side):
    return jnp.dot(left_side, right_side, precision=highest, preferred_element_type=jnp.float32)


def lowdot(left_side, right_side, left_dim, right_dim):
    return lax.dot_general(left_side, right_side, (((left_dim,), (right_dim,)), ((), ())), preferred_element_type=jnp.float32)


def silu_slope(pre_act):
    gate_value = jax.nn.sigmoid(pre_act)
    return gate_value * (1.0 + pre_act * (1.0 - gate_value))


def head_terms(source_head, upstream, decay_sums, step_rows, start_state, end_grad, skip_head, scores, in_map, out_map, in_wide, out_wide):
    length = decay_sums.shape[0]
    places = jnp.arange(length)
    causal = places[:, None] >= places[None, :]
    spread = decay_sums[:, None] - decay_sums[None, :]
    segment = jnp.where(causal, jnp.exp(jnp.where(causal, spread, 0.0)), 0.0)
    mixing = (segment * scores * step_rows[None, :]).astype(jnp.bfloat16)
    source_wide = source_head.astype(jnp.float32)
    upstream_wide = upstream.astype(jnp.float32)
    leading = jnp.exp(decay_sums)
    trailing = jnp.exp(decay_sums[-1] - decay_sums)
    output = lowdot(mixing, source_head, 1, 0) + leading[:, None] * product(out_wide, start_state.T) + skip_head * source_wide
    grad_source = lowdot(mixing, upstream, 0, 0) + (step_rows * trailing)[:, None] * product(in_wide, end_grad.T) + skip_head * upstream_wide
    pairing = lowdot(upstream, source_head, 1, 1)
    weighted = (segment * step_rows[None, :] * pairing).astype(jnp.bfloat16)
    grad_in = lowdot(weighted, out_map, 0, 0) + (step_rows * trailing)[:, None] * product(source_wide, end_grad)
    grad_out = lowdot(weighted, in_map, 1, 0) + leading[:, None] * product(upstream_wide, start_state)
    return output, grad_source, grad_in, grad_out


def block_carries(source, upstream, decay_sums, step_rows, in_wide, out_wide):
    remaining = jnp.exp(decay_sums[-1][None, :] - decay_sums)
    weighted_source = source.astype(jnp.float32) * (step_rows * remaining)[:, :, None]
    state_part = jnp.einsum("lhp,ln->hpn", weighted_source, in_wide, precision=highest)
    weighted_grad = upstream.astype(jnp.float32) * jnp.exp(decay_sums)[:, :, None]
    grad_part = jnp.einsum("lhp,ln->hpn", weighted_grad, out_wide, precision=highest)
    return state_part, grad_part


def block_terms(source, upstream, decay_sums, step_rows, in_map, out_map, start_states, end_grads, skip_gain):
    scores = jnp.dot(out_map, in_map.T, preferred_element_type=jnp.float32)
    in_wide = in_map.astype(jnp.float32)
    out_wide = out_map.astype(jnp.float32)

    def one_head(head_items):
        return head_terms(head_items[0], head_items[1], head_items[2], head_items[3], head_items[4], head_items[5], head_items[6], scores, in_map, out_map, in_wide, out_wide)

    outputs, grad_source, grad_in, grad_out = lax.map(one_head, (source.transpose(1, 0, 2), upstream.transpose(1, 0, 2), decay_sums.T, step_rows.T, start_states, end_grads, skip_gain))
    length = source.shape[0]
    outputs = outputs.transpose(1, 0, 2).reshape(length, -1)
    grad_source = grad_source.transpose(1, 0, 2).reshape(length, -1)
    return outputs, grad_source, jnp.sum(grad_in, 0), jnp.sum(grad_out, 0)


def forward_link(carry_state, link_items):
    return link_items[0][:, None, None] * carry_state + link_items[1], carry_state


def one_sequence(conv_input, in_state_map, out_state_map, step_size, grad_mixer, grad_output, decay_rate, skip_gain, conv_weight):
    tap_count = conv_weight.shape[0]
    length = conv_input.shape[0]
    channels = conv_input.shape[1]
    extended = jnp.concatenate([jnp.zeros((tap_count - 1, channels), jnp.float32), conv_input.astype(jnp.float32)], 0)
    pre_act = jnp.zeros((length, channels), jnp.float32)
    for offset in range(tap_count):
        pre_act = pre_act + conv_weight[offset] * extended[tap_count - 1 - offset: tap_count - 1 - offset + length]
    source = jax.nn.silu(pre_act).astype(jnp.bfloat16)
    blocks = length // TOK_DEV
    log_decay = -step_size * decay_rate[None, :]
    decay_sums = jnp.cumsum(log_decay.reshape(blocks, TOK_DEV, HEADS), axis=1)
    source_blocks = source.reshape(blocks, TOK_DEV, HEADS, HEAD_DIM)
    upstream_blocks = grad_mixer.reshape(blocks, TOK_DEV, HEADS, HEAD_DIM)
    step_blocks = step_size.reshape(blocks, TOK_DEV, HEADS)
    in_blocks = in_state_map.reshape(blocks, TOK_DEV, STATE)
    out_blocks = out_state_map.reshape(blocks, TOK_DEV, STATE)

    def carries_of(block_items):
        return block_carries(block_items[0], block_items[1], block_items[2], block_items[3], block_items[4].astype(jnp.float32), block_items[5].astype(jnp.float32))

    state_parts, grad_parts = lax.map(carries_of, (source_blocks, upstream_blocks, decay_sums, step_blocks, in_blocks, out_blocks))
    totals = jnp.exp(decay_sums[:, -1, :])
    zero_state = jnp.zeros((HEADS, HEAD_DIM, STATE), jnp.float32)
    unused, start_states = lax.scan(forward_link, zero_state, (totals, state_parts))
    unused, end_grads = lax.scan(forward_link, zero_state, (totals, grad_parts), reverse=True)

    def terms_of(block_items):
        return block_terms(block_items[0], block_items[1], block_items[2], block_items[3], block_items[4], block_items[5], block_items[6], block_items[7], skip_gain)

    outputs, grad_sources, grad_ins, grad_outs = lax.map(terms_of, (source_blocks, upstream_blocks, decay_sums, step_blocks, in_blocks, out_blocks, start_states, end_grads))
    mixer_out = outputs.reshape(length, channels).astype(jnp.bfloat16)
    grad_pre = grad_sources.reshape(length, channels) * silu_slope(pre_act)
    padded = jnp.concatenate([grad_pre, jnp.zeros((tap_count - 1, channels), jnp.float32)], 0)
    grad_input = jnp.zeros((length, channels), jnp.float32)
    for offset in range(tap_count):
        grad_input = grad_input + conv_weight[offset] * padded[offset: offset + length]
    weight_terms = jnp.stack([jnp.sum(grad_pre * extended[tap_count - 1 - offset: tap_count - 1 - offset + length], 0) for offset in range(tap_count)])
    proj_terms = lax.dot_general(grad_output, mixer_out, (((0,), (0,)), ((), ())), preferred_element_type=jnp.float32)
    return grad_input.astype(jnp.bfloat16), grad_ins.reshape(length, STATE).astype(jnp.bfloat16), grad_outs.reshape(length, STATE).astype(jnp.bfloat16), weight_terms, proj_terms


def reference(conv_input, in_state_map, out_state_map, step_size, decay_rate, skip_gain, conv_weight, grad_mixer, grad_output):
    def per_sequence(seq_items):
        return one_sequence(seq_items[0], seq_items[1], seq_items[2], seq_items[3], seq_items[4], seq_items[5], decay_rate, skip_gain, conv_weight)

    grad_input, grad_in, grad_out, weight_terms, proj_terms = lax.map(per_sequence, (conv_input, in_state_map, out_state_map, step_size, grad_mixer, grad_output))
    norm_scale = float(TOKENS) ** -0.5
    return grad_input, grad_in, grad_out, jnp.sum(weight_terms, 0) * norm_scale, jnp.sum(proj_terms, 0)
```

```python
import jax
import jax.numpy as jnp
from jax import lax
from jax.experimental import pallas as pl
from jax.experimental.pallas import tpu as pltpu
from jax.sharding import PartitionSpec as P

MESH = pl.DeviceIdType.MESH
F32 = jnp.float32
BF16 = jnp.bfloat16

NZ, NX, NC, NY = 8, 4, 2, 4
ROW = NX * NC
HEADS, HEAD_DIM, STATE = 4, 64, 128
TOK, INNER, TAPS = 256, 256, 4
SCALE = float(TOK * NZ * NX * NC * NY) ** -0.5
ORDER = (
    (2, 0), (0, 2), (2, 1), (1, 2), (2, 2), (2, 3), (3, 2), (1, 3),
    (3, 1), (3, 0), (0, 3), (1, 0), (0, 1), (1, 1), (3, 3), (0, 0),
)


class Counter:
    def __init__(self):
        self.used = 0

    def take(self, count=1):
        first = self.used
        self.used += count
        return first


def dot(a, b, da, db):
    return lax.dot_general(a, b, (((da,), (db,)), ((), ())), preferred_element_type=F32)


def exact(a, b, da, db):
    return lax.dot_general(
        a,
        b,
        (((da,), (db,)), ((), ())),
        precision=lax.Precision.HIGHEST,
        preferred_element_type=F32,
    )


def scan_slot(place, size, core):
    return place + core * (size - 1 - 2 * place)


def kernel(
    x_ref, b_ref, c_ref, step_ref, rate_ref, skip_ref, taps_ref, up_ref, g_ref,
    out_x, out_b, out_c, out_w, out_p,
    halo, ext, pre, src, ws, wg, lead, trail,
    tot, pieces, row_p, row_t, prefix, row_sum, row_log, z_p, z_t, z_state, back, states,
    loc_out, loc_src, loc_b, loc_c, mix, mix_peer,
    g_own, g_peer, gt,
    acc0, hold1, hold3, send2, relay, send1, send3, from_m, from_p, acc1, send_b, recv_b,
    part3, send_z, recv_z, grad_pre, w_row, w_y, w_z,
    g_sem, ssem, rsem,
):
    s = lax.axis_index("seq")
    y = lax.axis_index("dp")
    core = lax.rem(s, 2)
    x = lax.rem(lax.div(s, 2), 4)
    z = lax.div(s, ROW)
    j = lax.rem(s, ROW)
    count = Counter()
    waits = []

    def send(source, target, to, index, slot=None):
        copy = pltpu.make_async_remote_copy(
            src_ref=source,
            dst_ref=target,
            send_sem=ssem.at[index],
            recv_sem=rsem.at[index if slot is None else slot],
            device_id=to,
            device_id_type=MESH,
        )
        copy.start()
        return copy

    def arrived(target, slot):
        pltpu.make_async_remote_copy(
            src_ref=target,
            dst_ref=target,
            send_sem=ssem.at[0],
            recv_sem=rsem.at[slot],
            device_id=(s, y),
            device_id_type=MESH,
        ).wait_recv()

    def row_mate(d):
        other = lax.rem(j + d, ROW)
        return other, (z * ROW + other, y)

    def at_x(d):
        return ((z * NX + lax.rem(x + d, NX)) * NC + core, y)

    def at_y(d):
        return (s, lax.rem(y + d, NY))

    def at_z(d):
        other = lax.rem(z + d, NZ)
        return other, (other * ROW + j, y)

    peer = (s + 1 - 2 * core, y)
    following = (lax.rem(s + 1, NZ * ROW), y)
    previous = (lax.rem(s + NZ * ROW - 1, NZ * ROW), y)

    barrier = pltpu.get_barrier_semaphore()
    partners = [row_mate(d)[1] for d in range(1, ROW)]
    partners += [at_z(d)[1] for d in range(1, NZ)]
    partners += [at_y(d) for d in range(1, NY)]
    partners += [following, previous]
    for partner in partners:
        pl.semaphore_signal(barrier, inc=1, device_id=partner, device_id_type=MESH)

    @pl.loop(0, NZ * NX)
    def _(i):
        at = pl.multiple_of((i * NC + core) * 128, 128)
        pltpu.make_async_copy(g_ref.at[0, :, pl.ds(at, 128)], g_own.at[i], g_sem.at[0]).start()

    steps = step_ref[...]
    head_row = lax.broadcasted_iota(jnp.int32, (HEADS, TOK), 0)
    rates = jnp.full((HEADS, TOK), rate_ref[0], F32)
    for h in range(1, HEADS):
        rates = jnp.where(head_row == h, rate_ref[h], rates)
    token_r = lax.broadcasted_iota(jnp.int32, (TOK, TOK), 0)
    token_c = lax.broadcasted_iota(jnp.int32, (TOK, TOK), 1)
    upper = jnp.where(token_r <= token_c, 1.0, 0.0).astype(F32)
    sums = exact(-steps * rates, upper, 1, 0)
    rows = jnp.concatenate([sums, steps], axis=0)
    cols = rows.T
    head_of = lax.div(lax.broadcasted_iota(jnp.int32, (8, INNER), 1), HEAD_DIM)
    row_of = lax.broadcasted_iota(jnp.int32, (8, INNER), 0)
    sums_wide = exact(rows, jnp.where(row_of == head_of, 1.0, 0.0).astype(F32), 0, 0)
    step_wide = exact(rows, jnp.where(row_of == head_of + HEADS, 1.0, 0.0).astype(F32), 0, 0)
    lead[...] = jnp.exp(sums_wide)
    trail[...] = step_wide * jnp.exp(sums_wide[TOK - 1 : TOK, :] - sums_wide)
    tot[...] = jnp.broadcast_to(rows[:, TOK - 1 : TOK], (8, 128))
    upstream = up_ref[0]
    in_map = b_ref[0]
    out_map = c_ref[0]
    wg[...] = (upstream.astype(F32) * lead[...]).astype(BF16)
    grad_piece = dot(wg[...], out_map, 0, 0).astype(BF16)
    for h in range(HEADS):
        pieces[1, h] = grad_piece[h * HEAD_DIM : (h + 1) * HEAD_DIM]
    ext[16:, :] = x_ref[0].astype(F32)

    pl.semaphore_wait(barrier, len(partners))

    k = count.take()
    waits.append(send(x_ref.at[0, pl.ds(TOK - 16, 16), :], halo, following, k))

    slot_j = [scan_slot(j, ROW, c) for c in range(NC)]
    my_slot = scan_slot(j, ROW, core)
    total_at = count.take(ROW)
    row_t[my_slot] = tot[...]
    for d in range(1, ROW):
        other, to = row_mate(d)
        slot = scan_slot(j, ROW, lax.rem(other, 2))
        waits.append(send(tot, row_t.at[slot], to, total_at + d, total_at + slot))

    @pl.loop(0, NZ * NX)
    def _(i):
        at = pl.multiple_of((i * NC + 1 - core) * 128, 128)
        pltpu.make_async_remote_copy(
            src_ref=g_ref.at[0, :, pl.ds(at, 128)],
            dst_ref=g_peer.at[i],
            send_sem=g_sem.at[1],
            recv_sem=g_sem.at[2],
            device_id=peer,
            device_id_type=MESH,
        ).start()

    arrived(halo, k)
    first = jnp.where(s > 0, 1.0, 0.0)
    ext[0:16, :] = halo[...].astype(F32) * first
    value = jnp.zeros((TOK, INNER), F32)
    for tap in range(TAPS):
        value = value + taps_ref[tap : tap + 1, :] * ext[16 - tap : 16 - tap + TOK, :]
    pre[...] = value
    source = (value * jax.nn.sigmoid(value)).astype(BF16)
    src[...] = source
    ws[...] = (source.astype(F32) * trail[...]).astype(BF16)
    state_piece = dot(ws[...], in_map, 0, 0).astype(BF16)
    for h in range(HEADS):
        pieces[0, h] = state_piece[h * HEAD_DIM : (h + 1) * HEAD_DIM]

    piece_at = count.take(ROW)
    row_p[my_slot] = pieces[core, x]
    for d in range(1, ROW):
        other, to = row_mate(d)
        theirs = lax.rem(other, 2)
        slot = scan_slot(j, ROW, theirs)
        waits.append(
            send(pieces.at[theirs, lax.div(other, 2)], row_p.at[slot], to, piece_at + d, piece_at + slot)
        )

    scores = dot(out_map, in_map, 1, 1)
    causal = token_r >= token_c
    low = lax.broadcasted_iota(jnp.int32, (TOK, 128), 1) < HEAD_DIM
    for pair in range(HEADS // 2):
        lanes = slice(pair * 128, (pair + 1) * 128)
        sp = src[:, lanes]
        upp = up_ref[0, :, lanes]
        outs, grads = [], []
        for half in range(2):
            h = 2 * pair + half
            mine = low if half == 0 else jnp.logical_not(low)
            spread = cols[:, h : h + 1] - rows[h : h + 1, :]
            seg = jnp.where(causal, jnp.exp(jnp.where(causal, spread, 0.0)), 0.0)
            seg = seg * rows[HEADS + h : HEADS + h + 1, :]
            mixing = (seg * scores).astype(BF16)
            outs.append(dot(mixing, sp, 1, 0))
            grads.append(dot(mixing, upp, 0, 0))
            up_only = jnp.where(mine, upp.astype(F32), 0.0).astype(BF16)
            weighted = (seg * dot(up_only, sp, 1, 1)).astype(BF16)
            part_b = dot(weighted, out_map, 0, 0)
            part_c = dot(weighted, in_map, 1, 0)
            if h == 0:
                loc_b[...] = part_b
                loc_c[...] = part_c
            else:
                loc_b[...] += part_b
                loc_c[...] += part_c
        gain = jnp.where(low, skip_ref[2 * pair], skip_ref[2 * pair + 1])
        loc_out[:, lanes] = jnp.where(low, outs[0], outs[1]) + gain * sp.astype(F32)
        loc_src[:, lanes] = jnp.where(low, grads[0], grads[1]) + gain * upp.astype(F32)

    for d in range(1, ROW):
        slot = scan_slot(lax.rem(j + ROW - d, ROW), ROW, core)
        arrived(row_t.at[slot], total_at + slot)
        arrived(row_p.at[slot], piece_at + slot)
    running = jnp.zeros((HEAD_DIM, STATE), F32)
    decayed = jnp.zeros((1, 128), F32)
    before = []
    for q in range(ROW):
        prefix[q] = running
        before.append(decayed)
        own = row_t[q, pl.ds(x, 1), :]
        running = jnp.exp(own) * running + row_p[q].astype(F32)
        decayed = decayed + own
    row_sum[...] = running.astype(BF16)
    row_log[...] = jnp.broadcast_to(decayed, (8, 128))

    my_z = scan_slot(z, NZ, core)
    zs_at = count.take(NZ)
    zl_at = count.take(NZ)
    z_copies = []
    for d in range(1, NZ):
        other, to = at_z(d)
        later = scan_slot(other, NZ, core) > my_z
        pair_of = [
            pltpu.make_async_remote_copy(
                src_ref=source,
                dst_ref=target.at[my_z],
                send_sem=ssem.at[base + d],
                recv_sem=rsem.at[base + my_z],
                device_id=to,
                device_id_type=MESH,
            )
            for source, target, base in ((row_log, z_t, zl_at), (row_sum, z_p, zs_at))
        ]
        z_copies.append((later, pair_of))

        @pl.when(later)
        def _(pair_of=pair_of):
            for copy in pair_of:
                copy.start()

    def turned(held, column):
        @pl.loop(0, NZ * NX)
        def _(i):
            xi = lax.rem(i, NX)
            zi = pl.multiple_of(lax.div(i, NX) * 32, 32)
            block = held[i].T
            for yi in range(NY):
                gt[xi, yi, pl.ds(zi, 32), column : column + TOK] = block[yi * 32 : (yi + 1) * 32]

    pltpu.make_async_copy(g_own, g_own, g_sem.at[0]).wait()
    turned(g_own, 0)

    z_state[...] = jnp.zeros_like(z_state)
    for q in range(NZ - 1):

        @pl.when(q < my_z)
        def _(q=q):
            arrived(z_t.at[q], zl_at + q)
            arrived(z_p.at[q], zs_at + q)
            z_state[...] = jnp.exp(z_t[q, 0:1, :]) * z_state[...] + z_p[q].astype(F32)

    entering = z_state[...]
    for q in range(ROW):
        back[q] = (jnp.exp(before[q]) * entering + prefix[q]).astype(BF16)
    back_at = count.take(ROW)
    states[core, x] = back[my_slot]
    mine_at = back_at + core * NX + x
    for d in range(1, ROW):
        other, to = row_mate(d)
        slot = scan_slot(other, ROW, core)
        waits.append(send(back.at[slot], states.at[core, x], to, back_at + d, mine_at))

    g_both = pltpu.make_async_remote_copy(
        src_ref=g_peer, dst_ref=g_peer, send_sem=g_sem.at[1], recv_sem=g_sem.at[2],
        device_id=peer, device_id_type=MESH,
    )
    g_both.wait_recv()
    turned(g_peer, TOK)

    for d in range(1, ROW):
        other = lax.rem(j + ROW - d, ROW)
        c_of, x_of = lax.rem(other, 2), lax.div(other, 2)
        arrived(states.at[c_of, x_of], back_at + c_of * NX + x_of)
    start_state = states[0].reshape(INNER, STATE)
    end_grad = states[1].reshape(INNER, STATE)

    mix[...] = (loc_out[...] + lead[...] * dot(out_map, start_state, 1, 1)).astype(BF16)
    k = count.take()
    waits.append(send(mix, mix_peer, peer, k))
    mix_at = k

    grad_source = loc_src[...] + trail[...] * dot(in_map, end_grad, 1, 1)
    value = pre[...]
    gate = jax.nn.sigmoid(value)
    grad_value = grad_source * (gate * (1.0 + value * (1.0 - gate)))
    grad_pre[0:TOK, :] = grad_value
    k = count.take()
    halo_at = k
    waits.append(send(grad_pre.at[pl.ds(0, 8), :], grad_pre.at[pl.ds(TOK, 8), :], previous, k))
    terms = [
        jnp.sum(grad_value * ext[16 - tap : 16 - tap + TOK, :], axis=0, keepdims=True)
        for tap in range(TAPS)
    ]
    w_row[j] = jnp.concatenate(terms + [jnp.zeros((8 - TAPS, INNER), F32)], axis=0)
    w_at = count.take(ROW)
    for d in range(1, ROW):
        other, to = row_mate(d)
        waits.append(send(w_row.at[j], w_row.at[j], to, w_at + d, w_at + j))

    arrived(mix_peer, mix_at)

    axes = (at_x, at_y)
    far_at = [count.take(4) for _ in range(2)]
    one_at = [count.take(4) for _ in range(2)]
    three_at = [count.take(4) for _ in range(2)]
    both = jnp.concatenate([mix[...], mix_peer[...]], axis=0)

    def step_to(color, d):
        return axes[color](d)

    def handle(color, d, e, part):
        if d == 0:
            acc0[color, e] = part
        elif d == 2:
            send2[color, e] = part.astype(BF16)
            to = step_to(color, 1 if e < 2 else 3)
            waits.append(send(send2.at[color, e], relay.at[color, e], to, far_at[color] + e))
        elif d == 1 and e >= 2:
            send1[color, e] = part.astype(BF16)
            waits.append(send(send1.at[color, e], from_m.at[color, e], step_to(color, 1), one_at[color] + e))
        elif d == 3 and e < 2:
            send3[color, e] = part.astype(BF16)
            waits.append(send(send3.at[color, e], from_p.at[color, e], step_to(color, 3), three_at[color] + e))
        elif d == 1:
            hold1[color, e] = part
        else:
            hold3[color, e - 2] = part

    for dx, dy in ORDER:
        block = gt[lax.rem(x + dx, NX), lax.rem(y + dy, NY)]
        part = dot(block, both, 1, 0)
        handle(0, dx, dy, part[:, :128])
        handle(1, dy, dx, part[:, 128:])

    for e in (0, 1, 2, 3):
        for color in range(2):
            arrived(relay.at[color, e], far_at[color] + e)
            got = relay[color, e].astype(F32)
            if e < 2:
                send1[color, e] = (hold1[color, e] + got).astype(BF16)
                waits.append(send(send1.at[color, e], from_m.at[color, e], step_to(color, 1), one_at[color] + e))
            else:
                send3[color, e] = (hold3[color, e - 2] + got).astype(BF16)
                waits.append(send(send3.at[color, e], from_p.at[color, e], step_to(color, 3), three_at[color] + e))

    out_b[0] = (loc_b[...] + dot(ws[...], end_grad, 1, 0)).astype(BF16)
    out_c[0] = (loc_c[...] + dot(wg[...], start_state, 1, 0)).astype(BF16)
    arrived(grad_pre.at[pl.ds(TOK, 8), :], halo_at)
    last = jnp.where(s < NZ * ROW - 1, 1.0, 0.0)
    grad_pre[TOK : TOK + 8, :] = grad_pre[TOK : TOK + 8, :] * last
    value = jnp.zeros((TOK, INNER), F32)
    for tap in range(TAPS):
        value = value + taps_ref[tap : tap + 1, :] * grad_pre[tap : tap + TOK, :]
    out_x[0] = value.astype(BF16)

    wy_at = count.take(NY)
    for d in range(1, ROW):
        other = lax.rem(j + ROW - d, ROW)
        arrived(w_row.at[other], w_at + other)
    total = w_row[0]
    for q in range(1, ROW):
        total = total + w_row[q]
    w_y[y] = total
    for d in range(1, NY):
        waits.append(send(w_y.at[y], w_y.at[y], at_y(d), wy_at + d, wy_at + y))

    second_at = [count.take(4) for _ in range(2)]
    for e in (2, 1, 3, 0):
        for color in range(2):
            arrived(from_m.at[color, e], one_at[color] + e)
            arrived(from_p.at[color, e], three_at[color] + e)
            part = acc0[color, e] + from_m[color, e].astype(F32) + from_p[color, e].astype(F32)
            if e == 0:
                acc1[color] = part
            else:
                send_b[color, e] = part.astype(BF16)
                waits.append(
                    send(send_b.at[color, e], recv_b.at[color, e], axes[1 - color](e), second_at[color] + e)
                )

    wz_at = count.take(NZ)
    for d in range(1, NY):
        other = lax.rem(y + NY - d, NY)
        arrived(w_y.at[other], wy_at + other)
    total = w_y[0]
    for q in range(1, NY):
        total = total + w_y[q]
    w_z[z] = total
    for d in range(1, NZ):
        other, to = at_z(d)
        waits.append(send(w_z.at[z], w_z.at[z], to, wz_at + d, wz_at + z))

    for color in range(2):
        part = acc1[color]
        for e in range(1, 4):
            arrived(recv_b.at[color, e], second_at[color] + e)
            part = part + recv_b[color, e].astype(F32)
        for q in range(NZ):
            part3[q, :, color * 128 : (color + 1) * 128] = part[q * 32 : (q + 1) * 32]
            send_z[q, :, color * 128 : (color + 1) * 128] = part[q * 32 : (q + 1) * 32].astype(BF16)
    third_at = count.take(NZ)
    for d in range(1, NZ):
        other, to = at_z(d)
        waits.append(send(send_z.at[other], recv_z.at[d], to, third_at + d))

    for d in range(1, NZ):
        other = lax.rem(z + NZ - d, NZ)
        arrived(w_z.at[other], wz_at + other)
    total = w_z[0]
    for q in range(1, NZ):
        total = total + w_z[q]
    out_w[...] = total[0:TAPS] * SCALE

    final = part3[z]
    for d in range(1, NZ):
        arrived(recv_z.at[d], third_at + d)
        final = final + recv_z[d].astype(F32)
    out_p[...] = final

    g_both.wait_send()
    for later, pair_of in z_copies:

        @pl.when(later)
        def _(pair_of=pair_of):
            for copy in pair_of:
                copy.wait_send()

    for copy in waits:
        copy.wait_send()


SEMAPHORES = 192


def on_device(conv_input, in_map, out_map, step_size, decay_rate, skip_gain, conv_weight, grad_mixer, grad_output):
    vmem = pl.BlockSpec(memory_space=pltpu.VMEM)
    smem = pl.BlockSpec(memory_space=pltpu.SMEM)
    piece = (HEAD_DIM, STATE)
    half = (TOK, 128)
    scratch = [
        ((16, INNER), BF16), ((16 + TOK, INNER), F32), ((TOK, INNER), F32), ((TOK, INNER), BF16),
        ((TOK, INNER), BF16), ((TOK, INNER), BF16), ((TOK, INNER), F32), ((TOK, INNER), F32),
        ((8, 128), F32), ((2, HEADS, *piece), BF16), ((ROW, *piece), BF16), ((ROW, 8, 128), F32),
        ((ROW, *piece), F32), (piece, BF16), ((8, 128), F32), ((NZ, *piece), BF16), ((NZ, 8, 128), F32),
        (piece, F32), ((ROW, *piece), BF16), ((2, HEADS, *piece), BF16),
        ((TOK, INNER), F32), ((TOK, INNER), F32), ((TOK, STATE), F32), ((TOK, STATE), F32),
        ((TOK, INNER), BF16), ((TOK, INNER), BF16),
        ((NZ * NX, TOK, 128), BF16), ((NZ * NX, TOK, 128), BF16), ((NX, NY, TOK, 2 * TOK), BF16),
        ((2, 4, *half), F32), ((2, 2, *half), F32), ((2, 2, *half), F32), ((2, 4, *half), BF16),
        ((2, 4, *half), BF16), ((2, 4, *half), BF16), ((2, 4, *half), BF16), ((2, 4, *half), BF16),
        ((2, 4, *half), BF16), ((2, *half), F32), ((2, 4, *half), BF16), ((2, 4, *half), BF16),
        ((NZ, 32, INNER), F32), ((NZ, 32, INNER), BF16), ((NZ, 32, INNER), BF16),
        ((TOK + 8, INNER), F32), ((ROW, 8, INNER), F32), ((NY, 8, INNER), F32), ((NZ, 8, INNER), F32),
    ]
    return pl.pallas_call(
        kernel,
        name="mixer_backward",
        out_shape=(
            jax.ShapeDtypeStruct((1, TOK, INNER), BF16),
            jax.ShapeDtypeStruct((1, TOK, STATE), BF16),
            jax.ShapeDtypeStruct((1, TOK, STATE), BF16),
            jax.ShapeDtypeStruct((TAPS, INNER), F32),
            jax.ShapeDtypeStruct((32, INNER), F32),
        ),
        in_specs=[vmem, vmem, vmem, vmem, smem, smem, vmem, vmem, pl.BlockSpec(memory_space=pl.ANY)],
        out_specs=(vmem,) * 5,
        scratch_shapes=[
            *(pltpu.VMEM(shape, kind) for shape, kind in scratch),
            pltpu.SemaphoreType.DMA((3,)),
            pltpu.SemaphoreType.DMA((SEMAPHORES,)),
            pltpu.SemaphoreType.DMA((SEMAPHORES,)),
        ],
        compiler_params=pltpu.CompilerParams(
            collective_id=0, has_side_effects=True, vmem_limit_bytes=48 * 1024 * 1024
        ),
    )(conv_input, in_map, out_map, step_size[0].T, decay_rate, skip_gain, conv_weight, grad_mixer, grad_output)


def solution(mesh):
    split = P("dp", "seq", None)
    return jax.shard_map(
        on_device,
        mesh=mesh,
        in_specs=(split, split, split, split, P(), P(), P(), split, split),
        out_specs=(split, split, split, P(), P(("seq", "dp"), None)),
        check_vma=False,
    )
```

```python
import contextlib

import jax
import jax.numpy as jnp
from jax import lax
from jax.experimental import pallas as pl
from jax.experimental.pallas import tpu as pltpu
from jax.sharding import PartitionSpec as P

MESH = pl.DeviceIdType.MESH
F32 = jnp.float32
BF16 = jnp.bfloat16

NZ, NX, NC, NY = 8, 4, 2, 4
ROW = NX * NC
HEADS, HEAD_DIM, STATE = 4, 64, 128
TOK, INNER, TAPS = 256, 256, 4
EARLY = 6
SCALE = float(TOK * NZ * NX * NC * NY) ** -0.5
ORDER = (
    (2, 2), (2, 1), (1, 2), (2, 0), (0, 2), (2, 3), (3, 2), (1, 1),
    (1, 3), (3, 1), (3, 0), (0, 3), (0, 1), (1, 0), (3, 3), (0, 0),
)
PLUS, MINUS = (2, 0), (1, 3)
EARLY = 6
SCALE = float(TOK * NZ * NX * NC * NY) ** -0.5
ORDER = (
    (2, 0), (0, 2), (2, 1), (1, 2), (2, 2), (2, 3), (3, 2), (1, 3),
    (3, 1), (3, 0), (0, 3), (1, 0), (0, 1), (1, 1), (3, 3), (0, 0),
)


class Phases:
    def __init__(self):
        self.open = contextlib.ExitStack()

    def __call__(self, name):
        self.open.close()
        self.open.enter_context(jax.named_scope(name))


class Counter:
    def __init__(self):
        self.used = 0

    def take(self, count=1):
        first = self.used
        self.used += count
        return first


def dot(a, b, da, db):
    return lax.dot_general(a, b, (((da,), (db,)), ((), ())), preferred_element_type=F32)


def exact(a, b, da, db):
    return lax.dot_general(
        a,
        b,
        (((da,), (db,)), ((), ())),
        precision=lax.Precision.HIGHEST,
        preferred_element_type=F32,
    )


def scan_slot(place, size, core):
    return place + core * (size - 1 - 2 * place)


def kernel(
    x_hbm, b_hbm, c_hbm, step_hbm, rate_hbm, skip_hbm, taps_hbm, up_hbm, g_ref,
    x_out, b_out, c_out, w_out, p_out,
    out_x, out_b, out_c, out_w, out_p,
    x_ref, b_ref, c_ref, step_ref, taps_ref, up_ref, rate_ref, skip_ref,
    halo, ext, pre, src, ws, wg, lead, trail,
    tot, pieces, row_p, row_t, prefix, row_sum, row_log, z_p, z_t, z_state, back, states,
    begun, loc_out, loc_src, loc_b, loc_c, mix, mix_peer,
    g_own, g_peer, gt,
    acc0, hold1, hold3, send2, relay, send1, send3, from_m, from_p, acc1, send_b, recv_b,
    part3, send_z, recv_z, grad_pre, w_row, w_y, w_z,
    in_sem, out_sem, g_sem, ssem, rsem,
):
    phase = Phases()
    phase("entry")
    inputs = [
        pltpu.make_async_copy(source, target, in_sem.at[i])
        for i, (source, target) in enumerate(
            (
                (step_hbm, step_ref), (rate_hbm, rate_ref), (skip_hbm, skip_ref), (up_hbm.at[0], up_ref),
                (b_hbm.at[0], b_ref), (c_hbm.at[0], c_ref), (x_hbm.at[0], x_ref), (taps_hbm, taps_ref),
            )
        )
    ]
    outputs = [
        pltpu.make_async_copy(source, target, out_sem.at[i])
        for i, (source, target) in enumerate(
            (
                (out_x, x_out.at[0]), (out_b, b_out.at[0]), (out_c, c_out.at[0]),
                (out_w, w_out), (out_p, p_out),
            )
        )
    ]
    for copy in inputs:
        copy.start()
    s = lax.axis_index("seq")
    y = lax.axis_index("dp")
    core = lax.rem(s, 2)
    x = lax.rem(lax.div(s, 2), 4)
    z = lax.div(s, ROW)
    j = lax.rem(s, ROW)
    sends, count = Counter(), Counter()
    sent = []

    def remote(source, target, to, index, slot):
        return pltpu.make_async_remote_copy(
            src_ref=source,
            dst_ref=target,
            send_sem=ssem.at[index],
            recv_sem=rsem.at[slot],
            device_id=to,
            device_id_type=MESH,
        )

    def send(source, target, to, index, slot):
        remote(source, target, to, index, slot).start()

    def arrived(target, slot):
        remote(target, target, (s, y), 0, slot).wait_recv()

    def group(whole):
        index = sends.take()
        sent.append((whole, index))
        return index

    def row_mate(d):
        other = lax.rem(j + d, ROW)
        return other, (z * ROW + other, y)

    def at_x(d):
        return ((z * NX + lax.rem(x + d, NX)) * NC + core, y)

    def at_y(d):
        return (s, lax.rem(y + d, NY))

    def at_z(d):
        other = lax.rem(z + d, NZ)
        return other, (other * ROW + j, y)

    peer = (s + 1 - 2 * core, y)
    following = (lax.rem(s + 1, NZ * ROW), y)
    previous = (lax.rem(s + NZ * ROW - 1, NZ * ROW), y)

    barrier = pltpu.get_barrier_semaphore()
    partners = [row_mate(d)[1] for d in range(1, ROW)]
    partners += [at_z(d)[1] for d in range(1, NZ)]
    partners += [at_y(d) for d in range(1, NY)]
    partners += [following, previous]
    for partner in partners:
        pl.semaphore_signal(barrier, inc=1, device_id=partner, device_id_type=MESH)

    @pl.loop(0, NZ * NX)
    def _(i):
        at = pl.multiple_of((i * NC + core) * 128, 128)
        pltpu.make_async_copy(g_ref.at[0, :, pl.ds(at, 128)], g_own.at[i], g_sem.at[0]).start()

    phase("inputs")
    for copy in inputs:
        copy.wait()

    phase("decays")
    steps = step_ref[...]
    head_row = lax.broadcasted_iota(jnp.int32, (HEADS, TOK), 0)
    rates = jnp.full((HEADS, TOK), rate_ref[0], F32)
    for h in range(1, HEADS):
        rates = jnp.where(head_row == h, rate_ref[h], rates)
    token_r = lax.broadcasted_iota(jnp.int32, (TOK, TOK), 0)
    token_c = lax.broadcasted_iota(jnp.int32, (TOK, TOK), 1)
    upper = jnp.where(token_r <= token_c, 1.0, 0.0).astype(F32)
    sums = exact(-steps * rates, upper, 1, 0)
    rows = jnp.concatenate([sums, steps], axis=0)
    cols = rows.T
    head_of = lax.div(lax.broadcasted_iota(jnp.int32, (8, INNER), 1), HEAD_DIM)
    row_of = lax.broadcasted_iota(jnp.int32, (8, INNER), 0)
    sums_wide = exact(rows, jnp.where(row_of == head_of, 1.0, 0.0).astype(F32), 0, 0)
    step_wide = exact(rows, jnp.where(row_of == head_of + HEADS, 1.0, 0.0).astype(F32), 0, 0)
    lead[...] = jnp.exp(sums_wide)
    trail[...] = step_wide * jnp.exp(sums_wide[TOK - 1 : TOK, :] - sums_wide)
    tot[...] = jnp.broadcast_to(rows[:, TOK - 1 : TOK], (8, 128))
    upstream = up_ref[...]
    in_map = b_ref[...]
    out_map = c_ref[...]
    wg[...] = (upstream.astype(F32) * lead[...]).astype(BF16)
    grad_piece = dot(wg[...], out_map, 0, 0).astype(BF16)
    for h in range(HEADS):
        pieces[1, h] = grad_piece[h * HEAD_DIM : (h + 1) * HEAD_DIM]
    ext[0:16, :] = jnp.zeros((16, INNER), F32)
    ext[16:, :] = x_ref[...].astype(F32)

    phase("barrier")
    pl.semaphore_wait(barrier, len(partners))

    phase("sends")
    halo_at = count.take()
    halo_out = remote(x_ref.at[pl.ds(TOK - 16, 16), :], halo, following, sends.take(), halo_at)
    not_last, not_first = s < NZ * ROW - 1, s > 0

    @pl.when(not_last)
    def _():
        halo_out.start()

    slot_j = [scan_slot(j, ROW, c) for c in range(NC)]
    my_slot = scan_slot(j, ROW, core)
    total_at = count.take()
    total_out = group(row_t.at[pl.ds(0, ROW - 1)])
    row_t[my_slot] = tot[...]
    for d in range(1, ROW):
        other, to = row_mate(d)
        send(tot, row_t.at[scan_slot(j, ROW, lax.rem(other, 2))], to, total_out, total_at)

    piece_at = count.take()
    piece_out = group(row_p.at[pl.ds(0, ROW - 1)])

    def pieces_to(direction):
        @pl.when(core == direction)
        def _():
            row_p[my_slot] = pieces[direction, x]

        for d in range(NX):
            to_x = lax.rem(x + d, NX)
            copy = remote(
                pieces.at[direction, to_x],
                row_p.at[slot_j[direction]],
                ((z * NX + to_x) * NC + direction, y),
                piece_out,
                piece_at,
            )
            if d == 0:

                @pl.when(core != direction)
                def _():
                    copy.start()
            else:
                copy.start()

    guarded = [(not_last, [halo_out])]
    pieces_to(1)

    phase("conv")
    value = jnp.zeros((TOK, INNER), F32)
    for tap in range(TAPS):
        value = value + taps_ref[tap : tap + 1, :] * ext[16 - tap : 16 - tap + TOK, :]
    pre[...] = value

    phase("halo_wait")

    @pl.when(not_first)
    def _():
        arrived(halo, halo_at)
        ext[0:16, :] = halo[...].astype(F32)

    value = jnp.zeros((8, INNER), F32)
    for tap in range(TAPS):
        value = value + taps_ref[tap : tap + 1, :] * ext[16 - tap : 24 - tap, :]
    pre[0:8, :] = value

    phase("source")
    value = pre[...]
    source = (value * jax.nn.sigmoid(value)).astype(BF16)
    src[...] = source
    ws[...] = (source.astype(F32) * trail[...]).astype(BF16)
    state_piece = dot(ws[...], in_map, 0, 0).astype(BF16)
    for h in range(HEADS):
        pieces[0, h] = state_piece[h * HEAD_DIM : (h + 1) * HEAD_DIM]
    pieces_to(0)

    @pl.loop(0, NZ * NX)
    def _(i):
        at = pl.multiple_of((i * NC + 1 - core) * 128, 128)
        pltpu.make_async_remote_copy(
            src_ref=g_ref.at[0, :, pl.ds(at, 128)],
            dst_ref=g_peer.at[i],
            send_sem=g_sem.at[1],
            recv_sem=g_sem.at[2],
            device_id=peer,
            device_id_type=MESH,
        ).start()

    phase("inside")
    scores = dot(out_map, in_map, 1, 1)
    causal = token_r >= token_c
    low = lax.broadcasted_iota(jnp.int32, (TOK, 128), 1) < HEAD_DIM
    for pair in range(HEADS // 2):
        lanes = slice(pair * 128, (pair + 1) * 128)
        sp = src[:, lanes]
        upp = up_ref[:, lanes]
        outs, grads = [], []
        for half in range(2):
            h = 2 * pair + half
            mine = low if half == 0 else jnp.logical_not(low)
            spread = cols[:, h : h + 1] - rows[h : h + 1, :]
            seg = jnp.where(causal, jnp.exp(jnp.where(causal, spread, 0.0)), 0.0)
            seg = seg * rows[HEADS + h : HEADS + h + 1, :]
            mixing = (seg * scores).astype(BF16)
            outs.append(dot(mixing, sp, 1, 0))
            grads.append(dot(mixing, upp, 0, 0))
            up_only = jnp.where(mine, upp.astype(F32), 0.0).astype(BF16)
            weighted = (seg * dot(up_only, sp, 1, 1)).astype(BF16)
            part_b = dot(weighted, out_map, 0, 0)
            part_c = dot(weighted, in_map, 1, 0)
            if h == 0:
                loc_b[...] = part_b
                loc_c[...] = part_c
            else:
                loc_b[...] += part_b
                loc_c[...] += part_c
        gain = jnp.where(low, skip_ref[2 * pair], skip_ref[2 * pair + 1])
        loc_out[:, lanes] = jnp.where(low, outs[0], outs[1]) + gain * sp.astype(F32)
        loc_src[:, lanes] = jnp.where(low, grads[0], grads[1]) + gain * upp.astype(F32)

    phase("row_wait")
    arrived(row_t.at[pl.ds(0, ROW - 1)], total_at)
    arrived(row_p.at[pl.ds(0, ROW - 1)], piece_at)
    phase("row_scan")
    running = jnp.zeros((HEAD_DIM, STATE), F32)
    decayed = jnp.zeros((1, 128), F32)
    before = []
    for q in range(ROW):
        prefix[q] = running
        before.append(decayed)
        own = row_t[q, pl.ds(x, 1), :]
        running = jnp.exp(own) * running + row_p[q].astype(F32)
        decayed = decayed + own
    row_sum[...] = running.astype(BF16)
    row_log[...] = jnp.broadcast_to(decayed, (8, 128))

    my_z = scan_slot(z, NZ, core)
    zs_at = count.take(NZ - 1)
    zl_at = count.take(NZ - 1)
    for d in range(1, NZ):
        other, to = at_z(d)
        later = scan_slot(other, NZ, core) > my_z
        pair_of = [
            remote(source, target.at[my_z], to, sends.take(), base + my_z)
            for source, target, base in ((row_log, z_t, zl_at), (row_sum, z_p, zs_at))
        ]
        guarded.append((later, pair_of))

        @pl.when(later)
        def _(pair_of=pair_of):
            for copy in pair_of:
                copy.start()

    def turned(held, column):
        @pl.loop(0, NZ * NX)
        def _(i):
            xi = lax.rem(i, NX)
            zi = pl.multiple_of(lax.div(i, NX) * 32, 32)
            block = held[i].T
            for yi in range(NY):
                gt[xi, yi, pl.ds(zi, 32), column : column + TOK] = block[yi * 32 : (yi + 1) * 32]

    phase("turn_own")
    pltpu.make_async_copy(g_own, g_own, g_sem.at[0]).wait()
    turned(g_own, 0)

    phase("z_wait_scan")
    z_state[...] = jnp.zeros_like(z_state)
    for q in range(NZ - 1):

        @pl.when(q < my_z)
        def _(q=q):
            arrived(z_t.at[q], zl_at + q)
            arrived(z_p.at[q], zs_at + q)
            z_state[...] = jnp.exp(z_t[q, 0:1, :]) * z_state[...] + z_p[q].astype(F32)

    entering = z_state[...]
    for q in range(ROW):
        back[q] = (jnp.exp(before[q]) * entering + prefix[q]).astype(BF16)
    back_at = count.take()
    back_out = group(row_p.at[pl.ds(0, ROW - 1)])
    states[core, x] = back[my_slot]
    for d in range(1, ROW):
        other, to = row_mate(d)
        send(back.at[scan_slot(other, ROW, core)], states.at[core, x], to, back_out, back_at)

    g_both = pltpu.make_async_remote_copy(
        src_ref=g_peer, dst_ref=g_peer, send_sem=g_sem.at[1], recv_sem=g_sem.at[2],
        device_id=peer, device_id_type=MESH,
    )
    phase("turn_peer")
    g_both.wait_recv()
    turned(g_peer, TOK)

    phase("states_wait")
    arrived(row_p.at[pl.ds(0, ROW - 1)], back_at)
    start_state = states[0].reshape(INNER, STATE)
    end_grad = states[1].reshape(INNER, STATE)

    phase("mix")
    mix[...] = (loc_out[...] + lead[...] * dot(out_map, start_state, 1, 1)).astype(BF16)
    mix_at = count.take()
    send(mix, mix_peer, peer, group(mix), mix_at)

    phase("grad_pre")
    grad_source = loc_src[...] + trail[...] * dot(in_map, end_grad, 1, 1)
    value = pre[...]
    gate = jax.nn.sigmoid(value)
    grad_value = grad_source * (gate * (1.0 + value * (1.0 - gate)))
    grad_pre[0:TOK, :] = grad_value
    tail_at = count.take()
    tail_out = remote(
        grad_pre.at[pl.ds(0, 8), :], grad_pre.at[pl.ds(TOK, 8), :], previous, sends.take(), tail_at
    )
    guarded.append((not_first, [tail_out]))

    @pl.when(not_first)
    def _():
        tail_out.start()

    @pl.when(jnp.logical_not(not_last))
    def _():
        grad_pre[TOK : TOK + 8, :] = jnp.zeros((8, INNER), F32)

    terms = [
        jnp.sum(grad_value * ext[16 - tap : 16 - tap + TOK, :], axis=0, keepdims=True)
        for tap in range(TAPS)
    ]
    w_row[j] = jnp.concatenate(terms + [jnp.zeros((8 - TAPS, INNER), F32)], axis=0)
    w_at = count.take()
    w_out_at = group(w_row.at[pl.ds(0, ROW - 1)])
    for d in range(1, ROW):
        send(w_row.at[j], w_row.at[j], row_mate(d)[1], w_out_at, w_at)

    axes = (at_x, at_y)
    far_at = [count.take(4) for _ in range(2)]
    one_at = [count.take(4) for _ in range(2)]
    three_at = [count.take(4) for _ in range(2)]
    far_out, one_out, three_out = group(send2), group(send1), group(send3)
    def step_to(color, d):
        return axes[color](d)

    def handle(color, d, e, part):
        if d == 0:
            acc0[color, e] = part
        elif d == 2:
            send2[color, e] = part.astype(BF16)
            to = step_to(color, 1 if e in PLUS else 3)
            send(send2.at[color, e], relay.at[color, e], to, far_out, far_at[color] + e)
        elif d == 1 and e not in PLUS:
            send1[color, e] = part.astype(BF16)
            send(send1.at[color, e], from_m.at[color, e], step_to(color, 1), one_out, one_at[color] + e)
        elif d == 3 and e in PLUS:
            send3[color, e] = part.astype(BF16)
            send(send3.at[color, e], from_p.at[color, e], step_to(color, 3), three_out, three_at[color] + e)
        elif d == 1:
            hold1[color, PLUS.index(e)] = part
        else:
            hold3[color, MINUS.index(e)] = part

    def rows_of(dx, dy, column):
        return gt[lax.rem(x + dx, NX), lax.rem(y + dy, NY), :, column : column + TOK]

    phase("project_own")
    for i, (dx, dy) in enumerate(ORDER[:EARLY]):
        begun[i] = dot(rows_of(dx, dy, 0), mix[...], 1, 0)
    phase("mix_wait")
    arrived(mix_peer, mix_at)
    phase("project")
    for i, (dx, dy) in enumerate(ORDER):
        part = begun[i] if i < EARLY else dot(rows_of(dx, dy, 0), mix[...], 1, 0)
        part = part + dot(rows_of(dx, dy, TOK), mix_peer[...], 1, 0)
        handle(0, dx, dy, part[:, :128])
        handle(1, dy, dx, part[:, 128:])

    phase("relay")
    for e in (2, 1, 0, 3):
        for color in range(2):
            arrived(relay.at[color, e], far_at[color] + e)
            got = relay[color, e].astype(F32)
            if e in PLUS:
                send1[color, e] = (hold1[color, PLUS.index(e)] + got).astype(BF16)
                send(send1.at[color, e], from_m.at[color, e], step_to(color, 1), one_out, one_at[color] + e)
            else:
                send3[color, e] = (hold3[color, MINUS.index(e)] + got).astype(BF16)
                send(send3.at[color, e], from_p.at[color, e], step_to(color, 3), three_out, three_at[color] + e)

    phase("maps")
    out_b[...] = (loc_b[...] + dot(ws[...], end_grad, 1, 0)).astype(BF16)
    out_c[...] = (loc_c[...] + dot(wg[...], start_state, 1, 0)).astype(BF16)

    @pl.when(not_last)
    def _():
        arrived(grad_pre.at[pl.ds(TOK, 8), :], tail_at)

    value = jnp.zeros((TOK, INNER), F32)
    for tap in range(TAPS):
        value = value + taps_ref[tap : tap + 1, :] * grad_pre[tap : tap + TOK, :]
    out_x[...] = value.astype(BF16)
    for copy in outputs[:3]:
        copy.start()

    phase("taps_row")
    wy_at = count.take()
    wy_out = group(w_y.at[pl.ds(0, NY - 1)])
    arrived(w_row.at[pl.ds(0, ROW - 1)], w_at)
    total = w_row[0]
    for q in range(1, ROW):
        total = total + w_row[q]
    w_y[y] = total
    for d in range(1, NY):
        send(w_y.at[y], w_y.at[y], at_y(d), wy_out, wy_at)

    phase("stage1_wait")
    second_at = [count.take() for _ in range(2)]
    second_out = group(send_b.at[:, pl.ds(1, 3)])
    for e in (2, 1, 3, 0):
        for color in range(2):
            arrived(from_m.at[color, e], one_at[color] + e)
            arrived(from_p.at[color, e], three_at[color] + e)
            part = acc0[color, e] + from_m[color, e].astype(F32) + from_p[color, e].astype(F32)
            if e == 0:
                acc1[color] = part
            else:
                send_b[color, e] = part.astype(BF16)
                send(send_b.at[color, e], recv_b.at[color, e], axes[1 - color](e), second_out, second_at[color])

    phase("taps_y")
    wz_at = count.take()
    wz_out = group(w_z.at[pl.ds(0, NZ - 1)])
    arrived(w_y.at[pl.ds(0, NY - 1)], wy_at)
    total = w_y[0]
    for q in range(1, NY):
        total = total + w_y[q]
    w_z[z] = total
    for d in range(1, NZ):
        send(w_z.at[z], w_z.at[z], at_z(d)[1], wz_out, wz_at)

    phase("stage2_wait")
    for color in range(2):
        part = acc1[color]
        arrived(recv_b.at[color, pl.ds(1, 3)], second_at[color])
        for e in range(1, 4):
            part = part + recv_b[color, e].astype(F32)
        for q in range(NZ):
            part3[q, :, color * 128 : (color + 1) * 128] = part[q * 32 : (q + 1) * 32]
            send_z[q, :, color * 128 : (color + 1) * 128] = part[q * 32 : (q + 1) * 32].astype(BF16)
    third_at = count.take()
    third_out = group(send_z.at[pl.ds(0, NZ - 1)])
    for d in range(1, NZ):
        other, to = at_z(d)
        send(send_z.at[other], recv_z.at[d], to, third_out, third_at)

    phase("taps_z")
    arrived(w_z.at[pl.ds(0, NZ - 1)], wz_at)
    total = w_z[0]
    for q in range(1, NZ):
        total = total + w_z[q]
    out_w[...] = total[0:TAPS] * SCALE
    outputs[3].start()

    phase("stage3_wait")
    final = part3[z]
    arrived(recv_z.at[pl.ds(0, NZ - 1)], third_at)
    for d in range(1, NZ):
        final = final + recv_z[d].astype(F32)
    out_p[...] = final
    outputs[4].start()

    phase("drain")
    assert (sends.used, count.used) == (SENDS, ARRIVALS), (sends.used, count.used)
    g_both.wait_send()
    for later, pair_of in guarded:

        @pl.when(later)
        def _(pair_of=pair_of):
            for copy in pair_of:
                copy.wait_send()

    for whole, index in sent:
        remote(whole, whole, (s, y), index, 0).wait_send()
    for copy in outputs:
        copy.wait()
    phase.open.close()


def writer(*refs):
    n = (len(refs) - 2) // 3
    taken, given, held, sems = refs[:n], refs[n : 2 * n], refs[2 * n : 3 * n], refs[3 * n :]
    reads = [pltpu.make_async_copy(taken[i], held[i], sems[0].at[i]) for i in range(n)]
    writes = [pltpu.make_async_copy(held[i], given[i], sems[1].at[i]) for i in range(n)]
    for copy in reads:
        copy.start()
    for read, write in zip(reads, writes):
        read.wait()
        write.start()
    for copy in writes:
        copy.wait()


SENDS, ARRIVALS = 28, 50
VMEM_GRANT = 67043328


def on_device(conv_input, in_map, out_map, step_size, decay_rate, skip_gain, conv_weight, grad_mixer, grad_output):
    hbm = pl.BlockSpec(memory_space=pltpu.HBM)
    piece = (HEAD_DIM, STATE)
    half = (TOK, 128)
    scratch = [
        ((TOK, INNER), BF16), ((TOK, STATE), BF16), ((TOK, STATE), BF16), ((TAPS, INNER), F32), ((32, INNER), F32),
        ((TOK, INNER), BF16), ((TOK, STATE), BF16), ((TOK, STATE), BF16), ((HEADS, TOK), F32),
        ((TAPS, INNER), F32), ((TOK, INNER), BF16),
    ]
    scratch2 = [
        ((16, INNER), BF16), ((16 + TOK, INNER), F32), ((TOK, INNER), F32), ((TOK, INNER), BF16),
        ((TOK, INNER), BF16), ((TOK, INNER), BF16), ((TOK, INNER), F32), ((TOK, INNER), F32),
        ((8, 128), F32), ((2, HEADS, *piece), BF16), ((ROW, *piece), BF16), ((ROW, 8, 128), F32),
        ((ROW, *piece), F32), (piece, BF16), ((8, 128), F32), ((NZ, *piece), BF16), ((NZ, 8, 128), F32),
        (piece, F32), ((ROW, *piece), BF16), ((2, HEADS, *piece), BF16), ((EARLY, TOK, INNER), F32),
        ((TOK, INNER), F32), ((TOK, INNER), F32), ((TOK, STATE), F32), ((TOK, STATE), F32),
        ((TOK, INNER), BF16), ((TOK, INNER), BF16),
        ((NZ * NX, TOK, 128), BF16), ((NZ * NX, TOK, 128), BF16), ((NX, NY, TOK, 2 * TOK), BF16),
        ((2, 4, *half), F32), ((2, 2, *half), F32), ((2, 2, *half), F32), ((2, 4, *half), BF16),
        ((2, 4, *half), BF16), ((2, 4, *half), BF16), ((2, 4, *half), BF16), ((2, 4, *half), BF16),
        ((2, 4, *half), BF16), ((2, *half), F32), ((2, 4, *half), BF16), ((2, 4, *half), BF16),
        ((NZ, 32, INNER), F32), ((NZ, 32, INNER), BF16), ((NZ, 32, INNER), BF16),
        ((TOK + 8, INNER), F32), ((ROW, 8, INNER), F32), ((NY, 8, INNER), F32), ((NZ, 8, INNER), F32),
    ]
    outs = (
        jax.ShapeDtypeStruct((1, TOK, INNER), BF16),
        jax.ShapeDtypeStruct((1, TOK, STATE), BF16),
        jax.ShapeDtypeStruct((1, TOK, STATE), BF16),
        jax.ShapeDtypeStruct((TAPS, INNER), F32),
        jax.ShapeDtypeStruct((32, INNER), F32),
    )
    results = pl.pallas_call(
        kernel,
        name="mixer_backward",
        out_shape=outs,
        in_specs=[hbm] * 9,
        out_specs=(hbm,) * 5,
        scratch_shapes=[
            *(pltpu.VMEM(shape, kind) for shape, kind in scratch),
            pltpu.SMEM((HEADS,), F32),
            pltpu.SMEM((HEADS,), F32),
            *(pltpu.VMEM(shape, kind) for shape, kind in scratch2),
            pltpu.SemaphoreType.DMA((8,)),
            pltpu.SemaphoreType.DMA((5,)),
            pltpu.SemaphoreType.DMA((3,)),
            pltpu.SemaphoreType.DMA((SENDS,)),
            pltpu.SemaphoreType.DMA((ARRIVALS,)),
        ],
        compiler_params=pltpu.CompilerParams(
            collective_id=0, has_side_effects=True, vmem_limit_bytes=VMEM_GRANT
        ),
    )(conv_input, in_map, out_map, step_size[0].T, decay_rate, skip_gain, conv_weight, grad_mixer, grad_output)
    return pl.pallas_call(
        writer,
        name="writer",
        out_shape=outs,
        in_specs=[hbm] * 5,
        out_specs=(hbm,) * 5,
        scratch_shapes=[
            *(pltpu.VMEM(out.shape, out.dtype) for out in outs),
            pltpu.SemaphoreType.DMA((5,)),
            pltpu.SemaphoreType.DMA((5,)),
        ],
        compiler_params=pltpu.CompilerParams(vmem_limit_bytes=VMEM_GRANT),
    )(*results)


def solution(mesh):
    split = P("dp", "seq", None)
    return jax.shard_map(
        on_device,
        mesh=mesh,
        in_specs=(split, split, split, split, P(), P(), P(), split, split),
        out_specs=(split, split, split, P(), P(("seq", "dp"), None)),
        check_vma=False,
    )
```

```python
import contextlib

import jax
import jax.numpy as jnp
from jax import lax
from jax.experimental import pallas as pl
from jax.experimental.pallas import tpu as pltpu
from jax.sharding import PartitionSpec as P

MESH = pl.DeviceIdType.MESH
F32 = jnp.float32
BF16 = jnp.bfloat16

NZ, NX, NC, NY = 8, 4, 2, 4
ROW = NX * NC
HEADS, HEAD_DIM, STATE = 4, 64, 128
TOK, INNER, TAPS = 256, 256, 4
EARLY = 6
SCALE = float(TOK * NZ * NX * NC * NY) ** -0.5
ORDER = (
    (2, 2), (2, 1), (1, 2), (2, 0), (0, 2), (2, 3), (3, 2), (1, 1),
    (1, 3), (3, 1), (3, 0), (0, 3), (0, 1), (1, 0), (3, 3), (0, 0),
)
PLUS, MINUS = (2, 0), (1, 3)
EARLY = 6
SCALE = float(TOK * NZ * NX * NC * NY) ** -0.5
ORDER = (
    (2, 0), (0, 2), (2, 1), (1, 2), (2, 2), (2, 3), (3, 2), (1, 3),
    (3, 1), (3, 0), (0, 3), (1, 0), (0, 1), (1, 1), (3, 3), (0, 0),
)


class Phases:
    def __init__(self):
        self.open = contextlib.ExitStack()

    def __call__(self, name):
        self.open.close()
        self.open.enter_context(jax.named_scope(name))


class Counter:
    def __init__(self):
        self.used = 0

    def take(self, count=1):
        first = self.used
        self.used += count
        return first


def dot(a, b, da, db):
    return lax.dot_general(a, b, (((da,), (db,)), ((), ())), preferred_element_type=F32)


def exact(a, b, da, db):
    return lax.dot_general(
        a,
        b,
        (((da,), (db,)), ((), ())),
        precision=lax.Precision.HIGHEST,
        preferred_element_type=F32,
    )


def scan_slot(place, size, core):
    return place + core * (size - 1 - 2 * place)


def kernel(
    x_hbm, b_hbm, c_hbm, step_hbm, rate_hbm, skip_hbm, taps_hbm, up_hbm, g_ref,
    out_x, out_b, out_c, out_w, out_p,
    x_ref, b_ref, c_ref, step_ref, taps_ref, up_ref, rate_ref, skip_ref,
    halo, ext, pre, src, ws, wg, lead, trail,
    tot, pieces, row_p, row_t, prefix, row_sum, row_log, z_p, z_t, z_state, back, states,
    begun, loc_out, loc_src, loc_b, loc_c, mix, mix_peer,
    g_own, g_peer, gt,
    acc0, hold1, hold3, send2, relay, send1, send3, from_m, from_p, acc1, send_b, recv_b,
    part3, send_z, recv_z, grad_pre, w_row, w_y, w_z,
    in_sem, g_sem, ssem, rsem,
):
    phase = Phases()
    phase("entry")
    s = lax.axis_index("seq")
    y = lax.axis_index("dp")
    core = lax.rem(s, 2)
    x = lax.rem(lax.div(s, 2), 4)
    z = lax.div(s, ROW)
    j = lax.rem(s, ROW)
    sends, count = Counter(), Counter()
    sent = []

    def remote(source, target, to, index, slot):
        return pltpu.make_async_remote_copy(
            src_ref=source,
            dst_ref=target,
            send_sem=ssem.at[index],
            recv_sem=rsem.at[slot],
            device_id=to,
            device_id_type=MESH,
        )

    def send(source, target, to, index, slot):
        remote(source, target, to, index, slot).start()

    def arrived(target, slot):
        remote(target, target, (s, y), 0, slot).wait_recv()

    def group(whole):
        index = sends.take()
        sent.append((whole, index))
        return index

    def row_mate(d):
        other = lax.rem(j + d, ROW)
        return other, (z * ROW + other, y)

    def at_x(d):
        return ((z * NX + lax.rem(x + d, NX)) * NC + core, y)

    def at_y(d):
        return (s, lax.rem(y + d, NY))

    def at_z(d):
        other = lax.rem(z + d, NZ)
        return other, (other * ROW + j, y)

    peer = (s + 1 - 2 * core, y)
    following = (lax.rem(s + 1, NZ * ROW), y)
    previous = (lax.rem(s + NZ * ROW - 1, NZ * ROW), y)

    barrier = pltpu.get_barrier_semaphore()
    partners = [at_z(d)[1] for d in (4, 3, 5, 2, 6, 1, 7)]
    partners += [following, previous]
    partners += [row_mate(d)[1] for d in range(1, ROW)]
    partners += [at_y(d) for d in range(1, NY)]
    for partner in partners:
        pl.semaphore_signal(barrier, inc=1, device_id=partner, device_id_type=MESH)

    inputs = [
        pltpu.make_async_copy(source, target, in_sem.at[i])
        for i, (source, target) in enumerate(
            (
                (step_hbm, step_ref), (rate_hbm, rate_ref), (skip_hbm, skip_ref), (up_hbm.at[0], up_ref),
                (b_hbm.at[0], b_ref), (c_hbm.at[0], c_ref), (x_hbm.at[0], x_ref), (taps_hbm, taps_ref),
            )
        )
    ]
    for copy in inputs:
        copy.start()

    @pl.loop(0, NZ * NX)
    def _(i):
        at = pl.multiple_of((i * NC + core) * 128, 128)
        pltpu.make_async_copy(g_ref.at[0, :, pl.ds(at, 128)], g_own.at[i], g_sem.at[0]).start()

    phase("inputs")
    for copy in inputs:
        copy.wait()

    phase("barrier")
    pl.semaphore_wait(barrier, len(partners))

    phase("sends")
    halo_at = count.take()
    halo_out = remote(x_ref.at[pl.ds(TOK - 16, 16), :], halo, following, sends.take(), halo_at)
    not_last, not_first = s < NZ * ROW - 1, s > 0

    @pl.when(not_last)
    def _():
        halo_out.start()

    phase("decays")
    steps = step_ref[...]
    head_row = lax.broadcasted_iota(jnp.int32, (HEADS, TOK), 0)
    rates = jnp.full((HEADS, TOK), rate_ref[0], F32)
    for h in range(1, HEADS):
        rates = jnp.where(head_row == h, rate_ref[h], rates)
    token_r = lax.broadcasted_iota(jnp.int32, (TOK, TOK), 0)
    token_c = lax.broadcasted_iota(jnp.int32, (TOK, TOK), 1)
    upper = jnp.where(token_r <= token_c, 1.0, 0.0).astype(F32)
    sums = exact(-steps * rates, upper, 1, 0)
    rows = jnp.concatenate([sums, steps], axis=0)
    cols = rows.T
    head_of = lax.div(lax.broadcasted_iota(jnp.int32, (8, INNER), 1), HEAD_DIM)
    row_of = lax.broadcasted_iota(jnp.int32, (8, INNER), 0)
    sums_wide = exact(rows, jnp.where(row_of == head_of, 1.0, 0.0).astype(F32), 0, 0)
    step_wide = exact(rows, jnp.where(row_of == head_of + HEADS, 1.0, 0.0).astype(F32), 0, 0)
    lead[...] = jnp.exp(sums_wide)
    trail[...] = step_wide * jnp.exp(sums_wide[TOK - 1 : TOK, :] - sums_wide)
    tot[...] = jnp.broadcast_to(rows[:, TOK - 1 : TOK], (8, 128))
    upstream = up_ref[...]
    in_map = b_ref[...]
    out_map = c_ref[...]
    wg[...] = (upstream.astype(F32) * lead[...]).astype(BF16)
    grad_piece = dot(wg[...], out_map, 0, 0).astype(BF16)
    for h in range(HEADS):
        pieces[1, h] = grad_piece[h * HEAD_DIM : (h + 1) * HEAD_DIM]
    ext[0:16, :] = jnp.zeros((16, INNER), F32)
    ext[16:, :] = x_ref[...].astype(F32)

    slot_j = [scan_slot(j, ROW, c) for c in range(NC)]
    my_slot = scan_slot(j, ROW, core)
    total_at = count.take()
    total_out = group(row_t.at[pl.ds(0, ROW - 1)])
    row_t[my_slot] = tot[...]
    for d in range(1, ROW):
        other, to = row_mate(d)
        send(tot, row_t.at[scan_slot(j, ROW, lax.rem(other, 2))], to, total_out, total_at)

    piece_at = count.take()
    piece_out = group(row_p.at[pl.ds(0, ROW - 1)])

    def pieces_to(direction):
        @pl.when(core == direction)
        def _():
            row_p[my_slot] = pieces[direction, x]

        for d in range(NX):
            to_x = lax.rem(x + d, NX)
            copy = remote(
                pieces.at[direction, to_x],
                row_p.at[slot_j[direction]],
                ((z * NX + to_x) * NC + direction, y),
                piece_out,
                piece_at,
            )
            if d == 0:

                @pl.when(core != direction)
                def _():
                    copy.start()
            else:
                copy.start()

    guarded = [(not_last, [halo_out])]
    pieces_to(1)

    phase("conv")
    value = jnp.zeros((TOK, INNER), F32)
    for tap in range(TAPS):
        value = value + taps_ref[tap : tap + 1, :] * ext[16 - tap : 16 - tap + TOK, :]
    pre[...] = value

    phase("halo_wait")

    @pl.when(not_first)
    def _():
        arrived(halo, halo_at)
        ext[0:16, :] = halo[...].astype(F32)

    value = jnp.zeros((8, INNER), F32)
    for tap in range(TAPS):
        value = value + taps_ref[tap : tap + 1, :] * ext[16 - tap : 24 - tap, :]
    pre[0:8, :] = value

    phase("source")
    value = pre[...]
    source = (value * jax.nn.sigmoid(value)).astype(BF16)
    src[...] = source
    ws[...] = (source.astype(F32) * trail[...]).astype(BF16)
    state_piece = dot(ws[...], in_map, 0, 0).astype(BF16)
    for h in range(HEADS):
        pieces[0, h] = state_piece[h * HEAD_DIM : (h + 1) * HEAD_DIM]
    pieces_to(0)

    @pl.loop(0, NZ * NX)
    def _(i):
        at = pl.multiple_of((i * NC + 1 - core) * 128, 128)
        pltpu.make_async_remote_copy(
            src_ref=g_ref.at[0, :, pl.ds(at, 128)],
            dst_ref=g_peer.at[i],
            send_sem=g_sem.at[1],
            recv_sem=g_sem.at[2],
            device_id=peer,
            device_id_type=MESH,
        ).start()

    phase("inside")
    scores = dot(out_map, in_map, 1, 1)
    causal = token_r >= token_c
    low = lax.broadcasted_iota(jnp.int32, (TOK, 128), 1) < HEAD_DIM
    for pair in range(HEADS // 2):
        lanes = slice(pair * 128, (pair + 1) * 128)
        sp = src[:, lanes]
        upp = up_ref[:, lanes]
        outs, grads = [], []
        for half in range(2):
            h = 2 * pair + half
            mine = low if half == 0 else jnp.logical_not(low)
            spread = cols[:, h : h + 1] - rows[h : h + 1, :]
            seg = jnp.where(causal, jnp.exp(jnp.where(causal, spread, 0.0)), 0.0)
            seg = seg * rows[HEADS + h : HEADS + h + 1, :]
            mixing = (seg * scores).astype(BF16)
            outs.append(dot(mixing, sp, 1, 0))
            grads.append(dot(mixing, upp, 0, 0))
            up_only = jnp.where(mine, upp.astype(F32), 0.0).astype(BF16)
            weighted = (seg * dot(up_only, sp, 1, 1)).astype(BF16)
            part_b = dot(weighted, out_map, 0, 0)
            part_c = dot(weighted, in_map, 1, 0)
            if h == 0:
                loc_b[...] = part_b
                loc_c[...] = part_c
            else:
                loc_b[...] += part_b
                loc_c[...] += part_c
        gain = jnp.where(low, skip_ref[2 * pair], skip_ref[2 * pair + 1])
        loc_out[:, lanes] = jnp.where(low, outs[0], outs[1]) + gain * sp.astype(F32)
        loc_src[:, lanes] = jnp.where(low, grads[0], grads[1]) + gain * upp.astype(F32)

    phase("row_wait")
    arrived(row_t.at[pl.ds(0, ROW - 1)], total_at)
    arrived(row_p.at[pl.ds(0, ROW - 1)], piece_at)
    phase("row_scan")
    running = jnp.zeros((HEAD_DIM, STATE), F32)
    decayed = jnp.zeros((1, 128), F32)
    before = []
    for q in range(ROW):
        prefix[q] = running
        before.append(decayed)
        own = row_t[q, pl.ds(x, 1), :]
        running = jnp.exp(own) * running + row_p[q].astype(F32)
        decayed = decayed + own
    row_sum[...] = running.astype(BF16)
    row_log[...] = jnp.broadcast_to(decayed, (8, 128))

    my_z = scan_slot(z, NZ, core)
    zs_at = count.take(NZ - 1)
    zl_at = count.take(NZ - 1)
    for d in range(1, NZ):
        other, to = at_z(d)
        later = scan_slot(other, NZ, core) > my_z
        pair_of = [
            remote(source, target.at[my_z], to, sends.take(), base + my_z)
            for source, target, base in ((row_log, z_t, zl_at), (row_sum, z_p, zs_at))
        ]
        guarded.append((later, pair_of))

        @pl.when(later)
        def _(pair_of=pair_of):
            for copy in pair_of:
                copy.start()

    def turned(held, column):
        @pl.loop(0, NZ * NX)
        def _(i):
            xi = lax.rem(i, NX)
            zi = pl.multiple_of(lax.div(i, NX) * 32, 32)
            block = held[i].T
            for yi in range(NY):
                gt[xi, yi, pl.ds(zi, 32), column : column + TOK] = block[yi * 32 : (yi + 1) * 32]

    phase("turn_own")
    pltpu.make_async_copy(g_own, g_own, g_sem.at[0]).wait()
    turned(g_own, 0)

    phase("z_wait_scan")
    z_state[...] = jnp.zeros_like(z_state)
    for q in range(NZ - 1):

        @pl.when(q < my_z)
        def _(q=q):
            arrived(z_t.at[q], zl_at + q)
            arrived(z_p.at[q], zs_at + q)
            z_state[...] = jnp.exp(z_t[q, 0:1, :]) * z_state[...] + z_p[q].astype(F32)

    entering = z_state[...]
    for q in range(ROW):
        back[q] = (jnp.exp(before[q]) * entering + prefix[q]).astype(BF16)
    back_at = count.take()
    back_out = group(row_p.at[pl.ds(0, ROW - 1)])
    states[core, x] = back[my_slot]
    for d in range(1, ROW):
        other, to = row_mate(d)
        send(back.at[scan_slot(other, ROW, core)], states.at[core, x], to, back_out, back_at)

    g_both = pltpu.make_async_remote_copy(
        src_ref=g_peer, dst_ref=g_peer, send_sem=g_sem.at[1], recv_sem=g_sem.at[2],
        device_id=peer, device_id_type=MESH,
    )
    phase("turn_peer")
    g_both.wait_recv()
    turned(g_peer, TOK)

    phase("states_wait")
    arrived(row_p.at[pl.ds(0, ROW - 1)], back_at)
    start_state = states[0].reshape(INNER, STATE)
    end_grad = states[1].reshape(INNER, STATE)

    phase("mix")
    mix[...] = (loc_out[...] + lead[...] * dot(out_map, start_state, 1, 1)).astype(BF16)
    mix_at = count.take()
    send(mix, mix_peer, peer, group(mix), mix_at)

    phase("grad_pre")
    grad_source = loc_src[...] + trail[...] * dot(in_map, end_grad, 1, 1)
    value = pre[...]
    gate = jax.nn.sigmoid(value)
    grad_value = grad_source * (gate * (1.0 + value * (1.0 - gate)))
    grad_pre[0:TOK, :] = grad_value
    tail_at = count.take()
    tail_out = remote(
        grad_pre.at[pl.ds(0, 8), :], grad_pre.at[pl.ds(TOK, 8), :], previous, sends.take(), tail_at
    )
    guarded.append((not_first, [tail_out]))

    @pl.when(not_first)
    def _():
        tail_out.start()

    @pl.when(jnp.logical_not(not_last))
    def _():
        grad_pre[TOK : TOK + 8, :] = jnp.zeros((8, INNER), F32)

    terms = [
        jnp.sum(grad_value * ext[16 - tap : 16 - tap + TOK, :], axis=0, keepdims=True)
        for tap in range(TAPS)
    ]
    w_row[j] = jnp.concatenate(terms + [jnp.zeros((8 - TAPS, INNER), F32)], axis=0)
    w_at = count.take()
    w_out_at = group(w_row.at[pl.ds(0, ROW - 1)])
    for d in range(1, ROW):
        send(w_row.at[j], w_row.at[j], row_mate(d)[1], w_out_at, w_at)

    axes = (at_x, at_y)
    far_at = [count.take(4) for _ in range(2)]
    one_at = [count.take(4) for _ in range(2)]
    three_at = [count.take(4) for _ in range(2)]
    far_out, one_out, three_out = group(send2), group(send1), group(send3)
    def step_to(color, d):
        return axes[color](d)

    def handle(color, d, e, part):
        if d == 0:
            acc0[color, e] = part
        elif d == 2:
            send2[color, e] = part.astype(BF16)
            to = step_to(color, 1 if e in PLUS else 3)
            send(send2.at[color, e], relay.at[color, e], to, far_out, far_at[color] + e)
        elif d == 1 and e not in PLUS:
            send1[color, e] = part.astype(BF16)
            send(send1.at[color, e], from_m.at[color, e], step_to(color, 1), one_out, one_at[color] + e)
        elif d == 3 and e in PLUS:
            send3[color, e] = part.astype(BF16)
            send(send3.at[color, e], from_p.at[color, e], step_to(color, 3), three_out, three_at[color] + e)
        elif d == 1:
            hold1[color, PLUS.index(e)] = part
        else:
            hold3[color, MINUS.index(e)] = part

    def rows_of(dx, dy, column):
        return gt[lax.rem(x + dx, NX), lax.rem(y + dy, NY), :, column : column + TOK]

    phase("project_own")
    for i, (dx, dy) in enumerate(ORDER[:EARLY]):
        begun[i] = dot(rows_of(dx, dy, 0), mix[...], 1, 0)
    phase("mix_wait")
    arrived(mix_peer, mix_at)
    phase("project")
    for i, (dx, dy) in enumerate(ORDER):
        part = begun[i] if i < EARLY else dot(rows_of(dx, dy, 0), mix[...], 1, 0)
        part = part + dot(rows_of(dx, dy, TOK), mix_peer[...], 1, 0)
        handle(0, dx, dy, part[:, :128])
        handle(1, dy, dx, part[:, 128:])

    phase("relay")
    for e in (2, 1, 0, 3):
        for color in range(2):
            arrived(relay.at[color, e], far_at[color] + e)
            got = relay[color, e].astype(F32)
            if e in PLUS:
                send1[color, e] = (hold1[color, PLUS.index(e)] + got).astype(BF16)
                send(send1.at[color, e], from_m.at[color, e], step_to(color, 1), one_out, one_at[color] + e)
            else:
                send3[color, e] = (hold3[color, MINUS.index(e)] + got).astype(BF16)
                send(send3.at[color, e], from_p.at[color, e], step_to(color, 3), three_out, three_at[color] + e)

    phase("maps")
    out_b[0] = (loc_b[...] + dot(ws[...], end_grad, 1, 0)).astype(BF16)
    out_c[0] = (loc_c[...] + dot(wg[...], start_state, 1, 0)).astype(BF16)

    @pl.when(not_last)
    def _():
        arrived(grad_pre.at[pl.ds(TOK, 8), :], tail_at)

    value = jnp.zeros((TOK, INNER), F32)
    for tap in range(TAPS):
        value = value + taps_ref[tap : tap + 1, :] * grad_pre[tap : tap + TOK, :]
    out_x[0] = value.astype(BF16)

    phase("taps_row")
    wy_at = count.take()
    wy_out = group(w_y.at[pl.ds(0, NY - 1)])
    arrived(w_row.at[pl.ds(0, ROW - 1)], w_at)
    total = w_row[0]
    for q in range(1, ROW):
        total = total + w_row[q]
    w_y[y] = total
    for d in range(1, NY):
        send(w_y.at[y], w_y.at[y], at_y(d), wy_out, wy_at)

    phase("stage1_wait")
    second_at = [count.take() for _ in range(2)]
    second_out = group(send_b.at[:, pl.ds(1, 3)])
    for e in (2, 1, 3, 0):
        for color in range(2):
            arrived(from_m.at[color, e], one_at[color] + e)
            arrived(from_p.at[color, e], three_at[color] + e)
            part = acc0[color, e] + from_m[color, e].astype(F32) + from_p[color, e].astype(F32)
            if e == 0:
                acc1[color] = part
            else:
                send_b[color, e] = part.astype(BF16)
                send(send_b.at[color, e], recv_b.at[color, e], axes[1 - color](e), second_out, second_at[color])

    phase("taps_y")
    wz_at = count.take()
    wz_out = group(w_z.at[pl.ds(0, NZ - 1)])
    arrived(w_y.at[pl.ds(0, NY - 1)], wy_at)
    total = w_y[0]
    for q in range(1, NY):
        total = total + w_y[q]
    w_z[z] = total
    for d in range(1, NZ):
        send(w_z.at[z], w_z.at[z], at_z(d)[1], wz_out, wz_at)

    phase("stage2_wait")
    for color in range(2):
        part = acc1[color]
        arrived(recv_b.at[color, pl.ds(1, 3)], second_at[color])
        for e in range(1, 4):
            part = part + recv_b[color, e].astype(F32)
        for q in range(NZ):
            part3[q, :, color * 128 : (color + 1) * 128] = part[q * 32 : (q + 1) * 32]
            send_z[q, :, color * 128 : (color + 1) * 128] = part[q * 32 : (q + 1) * 32].astype(BF16)
    third_at = count.take()
    third_out = group(send_z.at[pl.ds(0, NZ - 1)])
    for d in range(1, NZ):
        other, to = at_z(d)
        send(send_z.at[other], recv_z.at[d], to, third_out, third_at)

    phase("taps_z")
    arrived(w_z.at[pl.ds(0, NZ - 1)], wz_at)
    total = w_z[0]
    for q in range(1, NZ):
        total = total + w_z[q]
    out_w[...] = total[0:TAPS] * SCALE

    phase("stage3_wait")
    final = part3[z]
    arrived(recv_z.at[pl.ds(0, NZ - 1)], third_at)
    for d in range(1, NZ):
        final = final + recv_z[d].astype(F32)
    out_p[...] = final

    phase("drain")
    assert (sends.used, count.used) == (SENDS, ARRIVALS), (sends.used, count.used)
    g_both.wait_send()
    for later, pair_of in guarded:

        @pl.when(later)
        def _(pair_of=pair_of):
            for copy in pair_of:
                copy.wait_send()

    for whole, index in sent:
        remote(whole, whole, (s, y), index, 0).wait_send()
    phase.open.close()


def writer(*refs):
    n = len(refs) // 2
    copies = [pltpu.make_async_copy(refs[i], refs[n + i], refs[-1].at[i]) for i in range(n)]
    for copy in copies:
        copy.start()
    for copy in copies:
        copy.wait()


SENDS, ARRIVALS = 28, 50
VMEM_GRANT = 32 * 1024 * 1024


def on_device(conv_input, in_map, out_map, step_size, decay_rate, skip_gain, conv_weight, grad_mixer, grad_output):
    hbm = pl.BlockSpec(memory_space=pltpu.HBM)
    vmem = pl.BlockSpec(memory_space=pltpu.VMEM)
    piece = (HEAD_DIM, STATE)
    half = (TOK, 128)
    scratch = [
        ((TOK, INNER), BF16), ((TOK, STATE), BF16), ((TOK, STATE), BF16), ((HEADS, TOK), F32),
        ((TAPS, INNER), F32), ((TOK, INNER), BF16),
    ]
    scratch2 = [
        ((16, INNER), BF16), ((16 + TOK, INNER), F32), ((TOK, INNER), F32), ((TOK, INNER), BF16),
        ((TOK, INNER), BF16), ((TOK, INNER), BF16), ((TOK, INNER), F32), ((TOK, INNER), F32),
        ((8, 128), F32), ((2, HEADS, *piece), BF16), ((ROW, *piece), BF16), ((ROW, 8, 128), F32),
        ((ROW, *piece), F32), (piece, BF16), ((8, 128), F32), ((NZ, *piece), BF16), ((NZ, 8, 128), F32),
        (piece, F32), ((ROW, *piece), BF16), ((2, HEADS, *piece), BF16), ((EARLY, TOK, INNER), F32),
        ((TOK, INNER), F32), ((TOK, INNER), F32), ((TOK, STATE), F32), ((TOK, STATE), F32),
        ((TOK, INNER), BF16), ((TOK, INNER), BF16),
        ((NZ * NX, TOK, 128), BF16), ((NZ * NX, TOK, 128), BF16), ((NX, NY, TOK, 2 * TOK), BF16),
        ((2, 4, *half), F32), ((2, 2, *half), F32), ((2, 2, *half), F32), ((2, 4, *half), BF16),
        ((2, 4, *half), BF16), ((2, 4, *half), BF16), ((2, 4, *half), BF16), ((2, 4, *half), BF16),
        ((2, 4, *half), BF16), ((2, *half), F32), ((2, 4, *half), BF16), ((2, 4, *half), BF16),
        ((NZ, 32, INNER), F32), ((NZ, 32, INNER), BF16), ((NZ, 32, INNER), BF16),
        ((TOK + 8, INNER), F32), ((ROW, 8, INNER), F32), ((NY, 8, INNER), F32), ((NZ, 8, INNER), F32),
    ]
    outs = (
        jax.ShapeDtypeStruct((1, TOK, INNER), BF16),
        jax.ShapeDtypeStruct((1, TOK, STATE), BF16),
        jax.ShapeDtypeStruct((1, TOK, STATE), BF16),
        jax.ShapeDtypeStruct((TAPS, INNER), F32),
        jax.ShapeDtypeStruct((32, INNER), F32),
    )
    given = [
        pltpu.with_memory_space_constraint(a, pltpu.HBM)
        for a in (
            conv_input, in_map, out_map, step_size[0].T, decay_rate, skip_gain, conv_weight, grad_mixer, grad_output
        )
    ]
    results = pl.pallas_call(
        kernel,
        name="mixer_backward",
        out_shape=outs,
        in_specs=[hbm] * 9,
        out_specs=(vmem,) * 5,
        scratch_shapes=[
            *(pltpu.VMEM(shape, kind) for shape, kind in scratch),
            pltpu.SMEM((HEADS,), F32),
            pltpu.SMEM((HEADS,), F32),
            *(pltpu.VMEM(shape, kind) for shape, kind in scratch2),
            pltpu.SemaphoreType.DMA((8,)),
            pltpu.SemaphoreType.DMA((3,)),
            pltpu.SemaphoreType.DMA((SENDS,)),
            pltpu.SemaphoreType.DMA((ARRIVALS,)),
        ],
        compiler_params=pltpu.CompilerParams(
            collective_id=0, has_side_effects=True, vmem_limit_bytes=VMEM_GRANT
        ),
    )(*given)
    return pl.pallas_call(
        writer,
        name="writer",
        out_shape=outs,
        in_specs=[vmem] * 5,
        out_specs=(hbm,) * 5,
        scratch_shapes=[pltpu.SemaphoreType.DMA((5,))],
        compiler_params=pltpu.CompilerParams(vmem_limit_bytes=1024 * 1024),
    )(*results)


def solution(mesh):
    split = P("dp", "seq", None)
    return jax.shard_map(
        on_device,
        mesh=mesh,
        in_specs=(split, split, split, split, P(), P(), P(), split, split),
        out_specs=(split, split, split, P(), P(("seq", "dp"), None)),
        check_vma=False,
    )
```

```python
import contextlib

import jax
import jax.numpy as jnp
from jax import lax
from jax.experimental import pallas as pl
from jax.experimental.pallas import tpu as pltpu
from jax.sharding import PartitionSpec as P

MESH = pl.DeviceIdType.MESH
F32 = jnp.float32
BF16 = jnp.bfloat16

NZ, NX, NC, NY = 8, 4, 2, 4
FAR_Z, FAR_Y, FAR_ROW = (4, 3, 5, 2, 6, 1, 7), (2, 1, 3), (4, 3, 5, 2, 6, 7, 1)
ROW = NX * NC
HEADS, HEAD_DIM, STATE = 4, 64, 128
TOK, INNER, TAPS = 256, 256, 4
EARLY = 6
SCALE = float(TOK * NZ * NX * NC * NY) ** -0.5
ORDER = (
    (2, 2), (2, 1), (1, 2), (2, 0), (0, 2), (2, 3), (3, 2), (1, 1),
    (1, 3), (3, 1), (3, 0), (0, 3), (0, 1), (1, 0), (3, 3), (0, 0),
)
PLUS, MINUS = (2, 0), (1, 3)
EARLY = 6
SCALE = float(TOK * NZ * NX * NC * NY) ** -0.5
ORDER = (
    (2, 0), (0, 2), (2, 1), (1, 2), (2, 2), (2, 3), (3, 2), (1, 3),
    (3, 1), (3, 0), (0, 3), (1, 0), (0, 1), (1, 1), (3, 3), (0, 0),
)


class Phases:
    def __init__(self):
        self.open = contextlib.ExitStack()

    def __call__(self, name):
        self.open.close()
        self.open.enter_context(jax.named_scope(name))


class Counter:
    def __init__(self):
        self.used = 0

    def take(self, count=1):
        first = self.used
        self.used += count
        return first


def dot(a, b, da, db):
    return lax.dot_general(a, b, (((da,), (db,)), ((), ())), preferred_element_type=F32)


def exact(a, b, da, db):
    return lax.dot_general(
        a,
        b,
        (((da,), (db,)), ((), ())),
        precision=lax.Precision.HIGHEST,
        preferred_element_type=F32,
    )


def scan_slot(place, size, core):
    return place + core * (size - 1 - 2 * place)


def kernel(
    x_hbm, b_hbm, c_hbm, step_hbm, rate_hbm, skip_hbm, taps_hbm, up_hbm, g_ref,
    out_x, out_b, out_c, out_w, out_p,
    x_ref, b_ref, c_ref, step_ref, taps_ref, up_ref, rate_ref, skip_ref,
    halo, ext, pre, src, ws, wg, lead, trail,
    tot, pieces, row_p, row_t, prefix, row_sum, row_log, z_p, z_t, z_state, back, states,
    begun, loc_out, loc_src, loc_b, loc_c, mix, mix_peer,
    g_own, g_peer, gt,
    acc0, hold1, hold3, send2, relay, send1, send3, came, acc1, send_b, recv_b,
    part3, send_z, recv_z, grad_pre, w_row, w_y, w_z,
    in_sem, g_sem, ssem, rsem,
):
    phase = Phases()
    phase("entry")
    s = lax.axis_index("seq")
    y = lax.axis_index("dp")
    core = lax.rem(s, 2)
    x = lax.rem(lax.div(s, 2), 4)
    z = lax.div(s, ROW)
    j = lax.rem(s, ROW)
    sends, count = Counter(), Counter()
    sent = []

    def remote(source, target, to, index, slot):
        return pltpu.make_async_remote_copy(
            src_ref=source,
            dst_ref=target,
            send_sem=ssem.at[index],
            recv_sem=rsem.at[slot],
            device_id=to,
            device_id_type=MESH,
        )

    def send(source, target, to, index, slot):
        remote(source, target, to, index, slot).start()

    def arrived(target, slot):
        remote(target, target, (s, y), 0, slot).wait_recv()

    def group(whole):
        index = sends.take()
        sent.append((whole, index))
        return index

    def row_mate(d):
        other = lax.rem(j + d, ROW)
        return other, (z * ROW + other, y)

    def at_x(d):
        return ((z * NX + lax.rem(x + d, NX)) * NC + core, y)

    def at_y(d):
        return (s, lax.rem(y + d, NY))

    def at_z(d):
        other = lax.rem(z + d, NZ)
        return other, (other * ROW + j, y)

    peer = (s + 1 - 2 * core, y)
    following = (lax.rem(s + 1, NZ * ROW), y)
    previous = (lax.rem(s + NZ * ROW - 1, NZ * ROW), y)

    barrier = pltpu.get_barrier_semaphore()
    partners = [at_z(d)[1] for d in FAR_Z]
    partners += [following, previous]
    partners += [row_mate(d)[1] for d in range(1, ROW)]
    partners += [at_y(d) for d in range(1, NY)]
    for partner in partners:
        pl.semaphore_signal(barrier, inc=1, device_id=partner, device_id_type=MESH)

    inputs = [
        pltpu.make_async_copy(source, target, in_sem.at[i])
        for i, (source, target) in enumerate(
            (
                (step_hbm, step_ref), (rate_hbm, rate_ref), (skip_hbm, skip_ref), (up_hbm.at[0], up_ref),
                (b_hbm.at[0], b_ref), (c_hbm.at[0], c_ref), (x_hbm.at[0], x_ref), (taps_hbm, taps_ref),
            )
        )
    ]
    for copy in inputs:
        copy.start()

    @pl.loop(0, NZ * NX)
    def _(i):
        at = pl.multiple_of((i * NC + core) * 128, 128)
        pltpu.make_async_copy(g_ref.at[0, :, pl.ds(at, 128)], g_own.at[i], g_sem.at[0]).start()

    phase("inputs")
    for copy in inputs:
        copy.wait()

    phase("barrier")
    pl.semaphore_wait(barrier, len(partners))

    phase("sends")
    halo_at = count.take()
    halo_out = remote(x_ref.at[pl.ds(TOK - 16, 16), :], halo, following, sends.take(), halo_at)
    not_last, not_first = s < NZ * ROW - 1, s > 0

    @pl.when(not_last)
    def _():
        halo_out.start()

    phase("decays")
    steps = step_ref[...]
    head_row = lax.broadcasted_iota(jnp.int32, (HEADS, TOK), 0)
    rates = jnp.full((HEADS, TOK), rate_ref[0], F32)
    for h in range(1, HEADS):
        rates = jnp.where(head_row == h, rate_ref[h], rates)
    token_r = lax.broadcasted_iota(jnp.int32, (TOK, TOK), 0)
    token_c = lax.broadcasted_iota(jnp.int32, (TOK, TOK), 1)
    upper = jnp.where(token_r <= token_c, 1.0, 0.0).astype(F32)
    sums = exact(-steps * rates, upper, 1, 0)
    rows = jnp.concatenate([sums, steps], axis=0)
    cols = rows.T
    head_of = lax.div(lax.broadcasted_iota(jnp.int32, (8, INNER), 1), HEAD_DIM)
    row_of = lax.broadcasted_iota(jnp.int32, (8, INNER), 0)
    sums_wide = exact(rows, jnp.where(row_of == head_of, 1.0, 0.0).astype(F32), 0, 0)
    step_wide = exact(rows, jnp.where(row_of == head_of + HEADS, 1.0, 0.0).astype(F32), 0, 0)
    lead[...] = jnp.exp(sums_wide)
    trail[...] = step_wide * jnp.exp(sums_wide[TOK - 1 : TOK, :] - sums_wide)
    tot[...] = jnp.broadcast_to(rows[:, TOK - 1 : TOK], (8, 128))
    upstream = up_ref[...]
    in_map = b_ref[...]
    out_map = c_ref[...]
    wg[...] = (upstream.astype(F32) * lead[...]).astype(BF16)
    grad_piece = dot(wg[...], out_map, 0, 0).astype(BF16)
    for h in range(HEADS):
        pieces[1, h] = grad_piece[h * HEAD_DIM : (h + 1) * HEAD_DIM]
    ext[0:16, :] = jnp.zeros((16, INNER), F32)
    ext[16:, :] = x_ref[...].astype(F32)

    slot_j = [scan_slot(j, ROW, c) for c in range(NC)]
    my_slot = scan_slot(j, ROW, core)
    total_at = count.take()
    total_out = group(row_t.at[pl.ds(0, ROW - 1)])
    row_t[my_slot] = tot[...]
    for d in FAR_ROW:
        other, to = row_mate(d)
        send(tot, row_t.at[scan_slot(j, ROW, lax.rem(other, 2))], to, total_out, total_at)

    piece_at = count.take()
    piece_out = group(row_p.at[pl.ds(0, ROW - 1)])

    def pieces_to(direction):
        @pl.when(core == direction)
        def _():
            row_p[my_slot] = pieces[direction, x]

        for d in (*FAR_Y, 0):
            to_x = lax.rem(x + d, NX)
            copy = remote(
                pieces.at[direction, to_x],
                row_p.at[slot_j[direction]],
                ((z * NX + to_x) * NC + direction, y),
                piece_out,
                piece_at,
            )
            if d == 0:

                @pl.when(core != direction)
                def _():
                    copy.start()
            else:
                copy.start()

    guarded = [(not_last, [halo_out])]
    pieces_to(1)

    phase("conv")
    value = jnp.zeros((TOK, INNER), F32)
    for tap in range(TAPS):
        value = value + taps_ref[tap : tap + 1, :] * ext[16 - tap : 16 - tap + TOK, :]
    pre[...] = value

    phase("halo_wait")

    @pl.when(not_first)
    def _():
        arrived(halo, halo_at)
        ext[0:16, :] = halo[...].astype(F32)

    value = jnp.zeros((8, INNER), F32)
    for tap in range(TAPS):
        value = value + taps_ref[tap : tap + 1, :] * ext[16 - tap : 24 - tap, :]
    pre[0:8, :] = value

    phase("source")
    value = pre[...]
    source = (value * jax.nn.sigmoid(value)).astype(BF16)
    src[...] = source
    ws[...] = (source.astype(F32) * trail[...]).astype(BF16)
    state_piece = dot(ws[...], in_map, 0, 0).astype(BF16)
    for h in range(HEADS):
        pieces[0, h] = state_piece[h * HEAD_DIM : (h + 1) * HEAD_DIM]
    pieces_to(0)

    @pl.loop(0, NZ * NX)
    def _(i):
        at = pl.multiple_of((i * NC + 1 - core) * 128, 128)
        pltpu.make_async_remote_copy(
            src_ref=g_ref.at[0, :, pl.ds(at, 128)],
            dst_ref=g_peer.at[i],
            send_sem=g_sem.at[1],
            recv_sem=g_sem.at[2],
            device_id=peer,
            device_id_type=MESH,
        ).start()

    phase("inside")
    scores = dot(out_map, in_map, 1, 1)
    causal = token_r >= token_c
    low = lax.broadcasted_iota(jnp.int32, (TOK, 128), 1) < HEAD_DIM
    for pair in range(HEADS // 2):
        lanes = slice(pair * 128, (pair + 1) * 128)
        sp = src[:, lanes]
        upp = up_ref[:, lanes]
        outs, grads = [], []
        for half in range(2):
            h = 2 * pair + half
            mine = low if half == 0 else jnp.logical_not(low)
            spread = cols[:, h : h + 1] - rows[h : h + 1, :]
            seg = jnp.where(causal, jnp.exp(jnp.where(causal, spread, 0.0)), 0.0)
            seg = seg * rows[HEADS + h : HEADS + h + 1, :]
            mixing = (seg * scores).astype(BF16)
            outs.append(dot(mixing, sp, 1, 0))
            grads.append(dot(mixing, upp, 0, 0))
            up_only = jnp.where(mine, upp.astype(F32), 0.0).astype(BF16)
            weighted = (seg * dot(up_only, sp, 1, 1)).astype(BF16)
            part_b = dot(weighted, out_map, 0, 0)
            part_c = dot(weighted, in_map, 1, 0)
            if h == 0:
                loc_b[...] = part_b
                loc_c[...] = part_c
            else:
                loc_b[...] += part_b
                loc_c[...] += part_c
        gain = jnp.where(low, skip_ref[2 * pair], skip_ref[2 * pair + 1])
        loc_out[:, lanes] = jnp.where(low, outs[0], outs[1]) + gain * sp.astype(F32)
        loc_src[:, lanes] = jnp.where(low, grads[0], grads[1]) + gain * upp.astype(F32)

    phase("row_wait")
    arrived(row_t.at[pl.ds(0, ROW - 1)], total_at)
    arrived(row_p.at[pl.ds(0, ROW - 1)], piece_at)
    phase("row_scan")
    running = jnp.zeros((HEAD_DIM, STATE), F32)
    decayed = jnp.zeros((1, 128), F32)
    before = []
    for q in range(ROW):
        prefix[q] = running
        before.append(decayed)
        own = row_t[q, pl.ds(x, 1), :]
        running = jnp.exp(own) * running + row_p[q].astype(F32)
        decayed = decayed + own
    row_sum[...] = running.astype(BF16)
    row_log[...] = jnp.broadcast_to(decayed, (8, 128))

    my_z = scan_slot(z, NZ, core)
    zs_at = count.take(NZ - 1)
    zl_at = count.take(NZ - 1)
    for d in FAR_Z:
        other, to = at_z(d)
        later = scan_slot(other, NZ, core) > my_z
        pair_of = [
            remote(source, target.at[my_z], to, sends.take(), base + my_z)
            for source, target, base in ((row_log, z_t, zl_at), (row_sum, z_p, zs_at))
        ]
        guarded.append((later, pair_of))

        @pl.when(later)
        def _(pair_of=pair_of):
            for copy in pair_of:
                copy.start()

    def turned(held, column):
        @pl.loop(0, NZ * NX)
        def _(i):
            xi = lax.rem(i, NX)
            zi = pl.multiple_of(lax.div(i, NX) * 32, 32)
            block = held[i].T
            for yi in range(NY):
                gt[xi, yi, pl.ds(zi, 32), column : column + TOK] = block[yi * 32 : (yi + 1) * 32]

    phase("turn_own")
    pltpu.make_async_copy(g_own, g_own, g_sem.at[0]).wait()
    turned(g_own, 0)

    phase("z_wait_scan")
    z_state[...] = jnp.zeros_like(z_state)
    for q in range(NZ - 1):

        @pl.when(q < my_z)
        def _(q=q):
            arrived(z_t.at[q], zl_at + q)
            arrived(z_p.at[q], zs_at + q)
            z_state[...] = jnp.exp(z_t[q, 0:1, :]) * z_state[...] + z_p[q].astype(F32)

    entering = z_state[...]
    for q in range(ROW):
        back[q] = (jnp.exp(before[q]) * entering + prefix[q]).astype(BF16)
    back_at = count.take()
    back_out = group(row_p.at[pl.ds(0, ROW - 1)])
    states[core, x] = back[my_slot]
    for d in FAR_ROW:
        other, to = row_mate(d)
        send(back.at[scan_slot(other, ROW, core)], states.at[core, x], to, back_out, back_at)

    g_both = pltpu.make_async_remote_copy(
        src_ref=g_peer, dst_ref=g_peer, send_sem=g_sem.at[1], recv_sem=g_sem.at[2],
        device_id=peer, device_id_type=MESH,
    )
    phase("turn_peer")
    g_both.wait_recv()
    turned(g_peer, TOK)

    phase("states_wait")
    arrived(row_p.at[pl.ds(0, ROW - 1)], back_at)
    start_state = states[0].reshape(INNER, STATE)
    end_grad = states[1].reshape(INNER, STATE)

    phase("mix")
    mix[...] = (loc_out[...] + lead[...] * dot(out_map, start_state, 1, 1)).astype(BF16)
    mix_at = count.take()
    send(mix, mix_peer, peer, group(mix), mix_at)

    phase("grad_pre")
    grad_source = loc_src[...] + trail[...] * dot(in_map, end_grad, 1, 1)
    value = pre[...]
    gate = jax.nn.sigmoid(value)
    grad_value = grad_source * (gate * (1.0 + value * (1.0 - gate)))
    grad_pre[0:TOK, :] = grad_value
    tail_at = count.take()
    tail_out = remote(
        grad_pre.at[pl.ds(0, 8), :], grad_pre.at[pl.ds(TOK, 8), :], previous, sends.take(), tail_at
    )
    guarded.append((not_first, [tail_out]))

    @pl.when(not_first)
    def _():
        tail_out.start()

    @pl.when(jnp.logical_not(not_last))
    def _():
        grad_pre[TOK : TOK + 8, :] = jnp.zeros((8, INNER), F32)

    terms = [
        jnp.sum(grad_value * ext[16 - tap : 16 - tap + TOK, :], axis=0, keepdims=True)
        for tap in range(TAPS)
    ]
    w_row[j] = jnp.concatenate(terms + [jnp.zeros((8 - TAPS, INNER), F32)], axis=0)
    w_at = count.take()
    w_out_at = group(w_row.at[pl.ds(0, ROW - 1)])
    for d in FAR_ROW:
        send(w_row.at[j], w_row.at[j], row_mate(d)[1], w_out_at, w_at)

    axes = (at_x, at_y)
    far_at = [count.take(4) for _ in range(2)]
    came_at = [count.take(4) for _ in range(2)]
    far_out, one_out, three_out = group(send2), group(send1), group(send3)
    def step_to(color, d):
        return axes[color](d)

    def ahead(color, e):
        send(send1.at[color, e], came.at[color, e, 0], step_to(color, 1), one_out, came_at[color] + e)

    def behind(color, e):
        send(send3.at[color, e], came.at[color, e, 1], step_to(color, 3), three_out, came_at[color] + e)

    def handle(color, d, e, part):
        if d == 0:
            acc0[color, e] = part
        elif d == 2:
            send2[color, e] = part.astype(BF16)
            to = step_to(color, 1 if e in PLUS else 3)
            send(send2.at[color, e], relay.at[color, e], to, far_out, far_at[color] + e)
        elif d == 1 and e not in PLUS:
            send1[color, e] = part.astype(BF16)
            if e != 3:
                ahead(color, e)
        elif d == 3 and e in PLUS:
            send3[color, e] = part.astype(BF16)
            if e != 0:
                behind(color, e)
        elif d == 1:
            hold1[color, PLUS.index(e)] = part
        else:
            hold3[color, MINUS.index(e)] = part

    def rows_of(dx, dy, column):
        return gt[lax.rem(x + dx, NX), lax.rem(y + dy, NY), :, column : column + TOK]

    phase("project_own")
    for i, (dx, dy) in enumerate(ORDER[:EARLY]):
        begun[i] = dot(rows_of(dx, dy, 0), mix[...], 1, 0)
    phase("mix_wait")
    arrived(mix_peer, mix_at)
    phase("project")
    for i, (dx, dy) in enumerate(ORDER):
        part = begun[i] if i < EARLY else dot(rows_of(dx, dy, 0), mix[...], 1, 0)
        part = part + dot(rows_of(dx, dy, TOK), mix_peer[...], 1, 0)
        handle(0, dx, dy, part[:, :128])
        handle(1, dy, dx, part[:, 128:])

    phase("relay")
    for e in (2, 1, 3, 0):
        for color in range(2):
            arrived(relay.at[color, e], far_at[color] + e)
            got = relay[color, e].astype(F32)
            if e in PLUS:
                send1[color, e] = (hold1[color, PLUS.index(e)] + got).astype(BF16)
                ahead(color, e)
            else:
                send3[color, e] = (hold3[color, MINUS.index(e)] + got).astype(BF16)
                behind(color, e)
            if e == 2:
                ahead(color, 3)
            elif e == 3:
                behind(color, 0)

    phase("maps")
    out_b[0] = (loc_b[...] + dot(ws[...], end_grad, 1, 0)).astype(BF16)
    out_c[0] = (loc_c[...] + dot(wg[...], start_state, 1, 0)).astype(BF16)

    @pl.when(not_last)
    def _():
        arrived(grad_pre.at[pl.ds(TOK, 8), :], tail_at)

    value = jnp.zeros((TOK, INNER), F32)
    for tap in range(TAPS):
        value = value + taps_ref[tap : tap + 1, :] * grad_pre[tap : tap + TOK, :]
    out_x[0] = value.astype(BF16)

    phase("taps_row")
    wy_at = count.take()
    wy_out = group(w_y.at[pl.ds(0, NY - 1)])
    arrived(w_row.at[pl.ds(0, ROW - 1)], w_at)
    total = w_row[0]
    for q in range(1, ROW):
        total = total + w_row[q]
    w_y[y] = total
    for d in FAR_Y:
        send(w_y.at[y], w_y.at[y], at_y(d), wy_out, wy_at)

    phase("stage1_wait")
    second_at = [count.take() for _ in range(2)]
    second_out = group(send_b.at[:, pl.ds(1, 3)])
    for e in (2, 1, 3, 0):
        for color in range(2):
            arrived(came.at[color, e], came_at[color] + e)
            part = acc0[color, e] + came[color, e, 0].astype(F32) + came[color, e, 1].astype(F32)
            if e == 0:
                acc1[color] = part
            else:
                send_b[color, e] = part.astype(BF16)
                send(send_b.at[color, e], recv_b.at[color, e], axes[1 - color](e), second_out, second_at[color])

    phase("taps_y")
    wz_at = count.take()
    wz_out = group(w_z.at[pl.ds(0, NZ - 1)])
    arrived(w_y.at[pl.ds(0, NY - 1)], wy_at)
    total = w_y[0]
    for q in range(1, NY):
        total = total + w_y[q]
    w_z[z] = total
    for d in FAR_Z:
        send(w_z.at[z], w_z.at[z], at_z(d)[1], wz_out, wz_at)

    phase("stage2_wait")
    for color in range(2):
        part = acc1[color]
        arrived(recv_b.at[color, pl.ds(1, 3)], second_at[color])
        for e in range(1, 4):
            part = part + recv_b[color, e].astype(F32)
        for q in range(NZ):
            part3[q, :, color * 128 : (color + 1) * 128] = part[q * 32 : (q + 1) * 32]
            send_z[q, :, color * 128 : (color + 1) * 128] = part[q * 32 : (q + 1) * 32].astype(BF16)
    third_at = count.take()
    third_out = group(send_z.at[pl.ds(0, NZ - 1)])
    for d in FAR_Z:
        other, to = at_z(d)
        send(send_z.at[other], recv_z.at[d], to, third_out, third_at)

    phase("taps_z")
    arrived(w_z.at[pl.ds(0, NZ - 1)], wz_at)
    total = w_z[0]
    for q in range(1, NZ):
        total = total + w_z[q]
    out_w[...] = total[0:TAPS] * SCALE

    phase("stage3_wait")
    final = part3[z]
    arrived(recv_z.at[pl.ds(0, NZ - 1)], third_at)
    for d in range(1, NZ):
        final = final + recv_z[d].astype(F32)
    out_p[...] = final

    phase("drain")
    assert (sends.used, count.used) == (SENDS, ARRIVALS), (sends.used, count.used)
    g_both.wait_send()
    for later, pair_of in guarded:

        @pl.when(later)
        def _(pair_of=pair_of):
            for copy in pair_of:
                copy.wait_send()

    for whole, index in sent:
        remote(whole, whole, (s, y), index, 0).wait_send()
    phase.open.close()


def writer(*refs):
    n = len(refs) // 2
    copies = [pltpu.make_async_copy(refs[i], refs[n + i], refs[-1].at[i]) for i in range(n)]
    for copy in copies:
        copy.start()
    for copy in copies:
        copy.wait()


SENDS, ARRIVALS = 28, 42
VMEM_GRANT = 32 * 1024 * 1024


def on_device(conv_input, in_map, out_map, step_size, decay_rate, skip_gain, conv_weight, grad_mixer, grad_output):
    hbm = pl.BlockSpec(memory_space=pltpu.HBM)
    vmem = pl.BlockSpec(memory_space=pltpu.VMEM)
    piece = (HEAD_DIM, STATE)
    half = (TOK, 128)
    scratch = [
        ((TOK, INNER), BF16), ((TOK, STATE), BF16), ((TOK, STATE), BF16), ((HEADS, TOK), F32),
        ((TAPS, INNER), F32), ((TOK, INNER), BF16),
    ]
    scratch2 = [
        ((16, INNER), BF16), ((16 + TOK, INNER), F32), ((TOK, INNER), F32), ((TOK, INNER), BF16),
        ((TOK, INNER), BF16), ((TOK, INNER), BF16), ((TOK, INNER), F32), ((TOK, INNER), F32),
        ((8, 128), F32), ((2, HEADS, *piece), BF16), ((ROW, *piece), BF16), ((ROW, 8, 128), F32),
        ((ROW, *piece), F32), (piece, BF16), ((8, 128), F32), ((NZ, *piece), BF16), ((NZ, 8, 128), F32),
        (piece, F32), ((ROW, *piece), BF16), ((2, HEADS, *piece), BF16), ((EARLY, TOK, INNER), F32),
        ((TOK, INNER), F32), ((TOK, INNER), F32), ((TOK, STATE), F32), ((TOK, STATE), F32),
        ((TOK, INNER), BF16), ((TOK, INNER), BF16),
        ((NZ * NX, TOK, 128), BF16), ((NZ * NX, TOK, 128), BF16), ((NX, NY, TOK, 2 * TOK), BF16),
        ((2, 4, *half), F32), ((2, 2, *half), F32), ((2, 2, *half), F32), ((2, 4, *half), BF16),
        ((2, 4, *half), BF16), ((2, 4, *half), BF16), ((2, 4, *half), BF16), ((2, 4, 2, *half), BF16),
        ((2, *half), F32), ((2, 4, *half), BF16), ((2, 4, *half), BF16),
        ((NZ, 32, INNER), F32), ((NZ, 32, INNER), BF16), ((NZ, 32, INNER), BF16),
        ((TOK + 8, INNER), F32), ((ROW, 8, INNER), F32), ((NY, 8, INNER), F32), ((NZ, 8, INNER), F32),
    ]
    outs = (
        jax.ShapeDtypeStruct((1, TOK, INNER), BF16),
        jax.ShapeDtypeStruct((1, TOK, STATE), BF16),
        jax.ShapeDtypeStruct((1, TOK, STATE), BF16),
        jax.ShapeDtypeStruct((TAPS, INNER), F32),
        jax.ShapeDtypeStruct((32, INNER), F32),
    )
    given = [
        pltpu.with_memory_space_constraint(a, pltpu.HBM)
        for a in (
            conv_input, in_map, out_map, step_size[0].T, decay_rate, skip_gain, conv_weight, grad_mixer, grad_output
        )
    ]
    results = pl.pallas_call(
        kernel,
        name="mixer_backward",
        out_shape=outs,
        in_specs=[hbm] * 9,
        out_specs=(vmem,) * 5,
        scratch_shapes=[
            *(pltpu.VMEM(shape, kind) for shape, kind in scratch),
            pltpu.SMEM((HEADS,), F32),
            pltpu.SMEM((HEADS,), F32),
            *(pltpu.VMEM(shape, kind) for shape, kind in scratch2),
            pltpu.SemaphoreType.DMA((8,)),
            pltpu.SemaphoreType.DMA((3,)),
            pltpu.SemaphoreType.DMA((SENDS,)),
            pltpu.SemaphoreType.DMA((ARRIVALS,)),
        ],
        compiler_params=pltpu.CompilerParams(
            collective_id=0, has_side_effects=True, vmem_limit_bytes=VMEM_GRANT
        ),
    )(*given)
    return pl.pallas_call(
        writer,
        name="writer",
        out_shape=outs,
        in_specs=[vmem] * 5,
        out_specs=(hbm,) * 5,
        scratch_shapes=[pltpu.SemaphoreType.DMA((5,))],
        compiler_params=pltpu.CompilerParams(vmem_limit_bytes=1024 * 1024),
    )(*results)


def solution(mesh):
    split = P("dp", "seq", None)
    return jax.shard_map(
        on_device,
        mesh=mesh,
        in_specs=(split, split, split, split, P(), P(), P(), split, split),
        out_specs=(split, split, split, P(), P(("seq", "dp"), None)),
        check_vma=False,
    )
```
